32 devices in a mesh: stage: 4 (over z), expert: 8 (over y, x, core).
Axes of the slice: x: 2, y: 2, z: 4, core: 2. Of those that a mesh axis runs over, the one named last changes fastest.
Arguments:
- x_act: bfloat16 [4, 8192, 1024], P('stage', 'expert')
- route_idx: int32 [4, 8192, 2], P('stage', 'expert')
- route_gate: float32 [4, 8192, 2], P('stage', 'expert')
- w_up: bfloat16 [4, 16, 1024, 1024], P('stage', 'expert')
- w_lin: bfloat16 [4, 16, 1024, 1024], P('stage', 'expert')
- w_down: bfloat16 [4, 16, 1024, 1024], P('stage', 'expert')
- dy_out: bfloat16 [4, 8192, 1024], P('stage', 'expert')
Outputs:
- output 1: bfloat16 [4, 8192, 1024], P('stage', 'expert')
- output 2: bfloat16 [4, 8192, 1024], P('stage', 'expert')
- output 3: bfloat16 [4, 16, 1024, 1024], P('stage', 'expert')
- output 4: bfloat16 [4, 16, 1024, 1024], P('stage', 'expert')
- output 5: bfloat16 [4, 16, 1024, 1024], P('stage', 'expert')
All inputs are finite; a program needn't handle non-finite values.
Results may differ from the reference program's by a relative error of at most 0.001.
Values are sent between devices in bfloat16 or wider.
A program may use at most 1 GiB of HBM per device.

```python
import jax
import jax.numpy as jnp
from jax import lax

STAGE_DEVS = 4
EXPERT_DEVS = 8
TOKENS = 1024
D_MODEL = 1024
D_FF = 1024
EXPERTS = 16
TOP_K = 2

CAPACITY = 4 * TOKENS // EXPERTS
ROWS = EXPERT_DEVS * TOKENS


def draw_routing(rng_key):
    key_hot, key_bias, key_cell, key_perm, key_swap = jax.random.split(rng_key, 5)
    num_cells = EXPERTS * CAPACITY
    cell_ids = jnp.arange(num_cells, dtype=jnp.int32)
    cell_expert = cell_ids // CAPACITY
    cell_slot = cell_ids % CAPACITY
    hot_expert = jax.random.randint(key_hot, (), 0, EXPERTS)
    expert_bias = jax.random.randint(key_bias, (EXPERTS,), 0, 4) * 256
    cell_score = jax.random.randint(key_cell, (num_cells,), 0, 1024) + expert_bias[cell_expert]
    needed = (cell_slot == 0) | (cell_expert == hot_expert)
    cell_score = jnp.where(needed, 4096, cell_score)
    top_vals, chosen = lax.top_k(cell_score * num_cells + cell_ids, 2 * TOKENS)
    chosen_expert = jnp.sort(chosen) // CAPACITY
    expert_pairs = jnp.stack([chosen_expert[:TOKENS], chosen_expert[TOKENS:]], axis=1)
    expert_pairs = expert_pairs[jax.random.permutation(key_perm, TOKENS)]
    swap_flag = jax.random.randint(key_swap, (TOKENS, 1), 0, 2)
    return jnp.where(swap_flag == 1, expert_pairs[:, ::-1], expert_pairs).astype(jnp.int32)


def setup_inputs(seed: int = 0) -> dict:
    root_key = jax.random.key(seed)
    key_x, key_route, key_gate, key_up, key_lin, key_down, key_dy = jax.random.split(root_key, 7)
    shape_tok = (STAGE_DEVS, ROWS, D_MODEL)
    x_act = jax.random.normal(key_x, shape_tok, jnp.float32).astype(jnp.bfloat16)
    route_keys = jax.random.split(key_route, STAGE_DEVS * EXPERT_DEVS)
    route_idx = jax.vmap(draw_routing)(route_keys).reshape(STAGE_DEVS, ROWS, TOP_K)
    first_gate = jax.random.uniform(key_gate, (STAGE_DEVS, ROWS, 1), jnp.float32, 0.3, 0.7)
    route_gate = jnp.concatenate([first_gate, 1.0 - first_gate], axis=-1)
    shape_in = (STAGE_DEVS, EXPERTS, D_MODEL, D_FF)
    shape_out = (STAGE_DEVS, EXPERTS, D_FF, D_MODEL)
    w_up = (jax.random.normal(key_up, shape_in, jnp.float32) * D_MODEL ** -0.5).astype(jnp.bfloat16)
    w_lin = (jax.random.normal(key_lin, shape_in, jnp.float32) * D_MODEL ** -0.5).astype(jnp.bfloat16)
    w_down = (jax.random.normal(key_down, shape_out, jnp.float32) * D_FF ** -0.5).astype(jnp.bfloat16)
    dy_out = jax.random.normal(key_dy, shape_tok, jnp.float32).astype(jnp.bfloat16)
    return {"x_act": x_act, "route_idx": route_idx, "route_gate": route_gate, "w_up": w_up, "w_lin": w_lin, "w_down": w_down, "dy_out": dy_out}


def expert_block(x_src, idx_src, gate_src, dy_dst, w_up, w_lin, w_down):
    member = jnp.sum(jax.nn.one_hot(idx_src, EXPERTS, dtype=jnp.int32), axis=1)
    earlier = jnp.cumsum(member, axis=0) - member
    slot_pos = jnp.take_along_axis(earlier, idx_src, axis=1)
    x_copies = jnp.broadcast_to(x_src.astype(jnp.float32)[:, None, :], (TOKENS, TOP_K, D_MODEL))
    empty_rows = jnp.zeros((EXPERTS, CAPACITY, D_MODEL), jnp.float32)
    x_rows = empty_rows.at[idx_src, slot_pos].set(x_copies)
    pre_up = jnp.einsum("ecd,edf->ecf", x_rows, w_up)
    pre_lin = jnp.einsum("ecd,edf->ecf", x_rows, w_lin)
    act_up = jax.nn.silu(pre_up)
    hidden = (act_up * pre_lin).astype(jnp.bfloat16).astype(jnp.float32)
    out_rows = jnp.einsum("ecf,efd->ecd", hidden, w_down).astype(jnp.bfloat16).astype(jnp.float32)
    out_copies = out_rows[idx_src, slot_pos]
    y_tok = jnp.sum(gate_src[:, :, None] * out_copies, axis=1).astype(jnp.bfloat16)
    d_copies = (gate_src[:, :, None] * dy_dst.astype(jnp.float32)[:, None, :]).astype(jnp.bfloat16).astype(jnp.float32)
    d_rows = empty_rows.at[idx_src, slot_pos].set(d_copies)
    d_hidden = jnp.einsum("ecd,efd->ecf", d_rows, w_down).astype(jnp.bfloat16).astype(jnp.float32)
    sigmoid_up = jax.nn.sigmoid(pre_up)
    d_up = (d_hidden * pre_lin * sigmoid_up * (1.0 + pre_up * (1.0 - sigmoid_up))).astype(jnp.bfloat16).astype(jnp.float32)
    d_lin = (d_hidden * act_up).astype(jnp.bfloat16).astype(jnp.float32)
    g_up = jnp.einsum("ecd,ecf->edf", x_rows, d_up)
    g_lin = jnp.einsum("ecd,ecf->edf", x_rows, d_lin)
    g_down = jnp.einsum("ecf,ecd->efd", hidden, d_rows)
    dx_rows = (jnp.einsum("ecf,edf->ecd", d_up, w_up) + jnp.einsum("ecf,edf->ecd", d_lin, w_lin)).astype(jnp.bfloat16).astype(jnp.float32)
    dx_tok = jnp.sum(dx_rows[idx_src, slot_pos], axis=1).astype(jnp.bfloat16)
    return y_tok, dx_tok, g_up, g_lin, g_down


def stage_block(stage_args):
    x_stage, idx_stage, gate_stage, dy_stage, w_up, w_lin, w_down = stage_args
    w_up32 = w_up.astype(jnp.float32)
    w_lin32 = w_lin.astype(jnp.float32)
    w_down32 = w_down.astype(jnp.float32)

    def device_step(grad_sums, dev_block):
        block_out = expert_block(dev_block[0], dev_block[1], dev_block[2], dev_block[3], w_up32, w_lin32, w_down32)
        new_sums = (grad_sums[0] + block_out[2], grad_sums[1] + block_out[3], grad_sums[2] + block_out[4])
        return new_sums, (block_out[0], block_out[1])

    zero_grads = (jnp.zeros((EXPERTS, D_MODEL, D_FF), jnp.float32), jnp.zeros((EXPERTS, D_MODEL, D_FF), jnp.float32), jnp.zeros((EXPERTS, D_FF, D_MODEL), jnp.float32))
    dev_blocks = (x_stage.reshape(EXPERT_DEVS, TOKENS, D_MODEL), idx_stage.reshape(EXPERT_DEVS, TOKENS, TOP_K), gate_stage.reshape(EXPERT_DEVS, TOKENS, TOP_K), dy_stage.reshape(EXPERT_DEVS, TOKENS, D_MODEL))
    grad_sums, tok_outs = lax.scan(device_step, zero_grads, dev_blocks)
    y_stage = tok_outs[0].reshape(ROWS, D_MODEL)
    dx_stage = tok_outs[1].reshape(ROWS, D_MODEL)
    return y_stage, dx_stage, grad_sums[0].astype(jnp.bfloat16), grad_sums[1].astype(jnp.bfloat16), grad_sums[2].astype(jnp.bfloat16)


def reference(x_act, route_idx, route_gate, w_up, w_lin, w_down, dy_out):
    x_from = jnp.roll(x_act, 1, axis=0)
    idx_from = jnp.roll(route_idx, 1, axis=0)
    gate_from = jnp.roll(route_gate, 1, axis=0)
    y_out, dx_next, dw_up, dw_lin, dw_down = lax.map(stage_block, (x_from, idx_from, gate_from, dy_out, w_up, w_lin, w_down))
    dx_act = jnp.roll(dx_next, -1, axis=0)
    return y_out, dx_act, dw_up, dw_lin, dw_down
```

```python
import jax
import jax.numpy as jnp
from jax import lax
from jax.sharding import PartitionSpec as P

F32 = jnp.float32
BF16 = jnp.bfloat16


def earlier_counts(member):
    tokens = member.shape[-1]
    tok_ids = jnp.arange(tokens, dtype=jnp.int32)
    before = (tok_ids[:, None] < tok_ids[None, :]).astype(BF16)
    return jnp.dot(member.astype(BF16), before, preferred_element_type=F32).astype(jnp.int32)


def solution(mesh):
    stages = mesh.shape["stage"]
    groups = mesh.shape["expert"]
    send_next = [(src, (src + 1) % stages) for src in range(stages)]
    send_back = [(src, (src - 1) % stages) for src in range(stages)]
    tok_spec = P("stage", "expert", None)
    w_spec = P("stage", "expert", None, None)

    def device_step(x_act, route_idx, route_gate, w_up, w_lin, w_down, dy_out):
        tokens = x_act.shape[1]
        local = w_up.shape[1]
        num_experts = local * groups
        capacity = 4 * tokens // num_experts
        slots = jnp.arange(capacity, dtype=jnp.int32)

        meta = jnp.concatenate([route_idx[0].T.astype(F32), route_gate[0].T], axis=0)
        meta = lax.ppermute(meta, "stage", send_next)
        x_tok = lax.ppermute(x_act[0], "stage", send_next)
        meta_all = lax.all_gather(meta, "expert")
        dy_all = lax.all_gather(dy_out[0], "expert")
        x_all = lax.all_gather(x_tok, "expert")

        first = lax.axis_index("expert") * local
        idx_all = meta_all[:, :2].astype(jnp.int32)
        gate_all = meta_all[:, 2:]
        mine = idx_all[:, None] == (first + jnp.arange(local, dtype=jnp.int32))[None, :, None, None]
        member = jnp.any(mine, axis=2)
        gate_m = jnp.sum(jnp.where(mine, gate_all[:, None], 0.0), axis=2)
        pos = earlier_counts(member.reshape(groups * local, tokens)).reshape(groups, local, tokens)
        pos = jnp.where(member, pos, -1)
        hot = pos[:, :, None, :] == slots[None, None, :, None]
        slot_gate = jnp.sum(jnp.where(hot, gate_m[:, :, None, :], 0.0), axis=3)
        hot = hot.astype(BF16)

        idx_own = meta[:2].astype(jnp.int32)
        gate_own = meta[2:]
        is_exp = idx_own[:, None, :] == jnp.arange(num_experts, dtype=jnp.int32)[None, :, None]
        pos_own = earlier_counts(jnp.any(is_exp, axis=0))
        slot_own = jnp.sum(jnp.where(is_exp, pos_own[None], 0), axis=1)
        dev_own = idx_own // local
        loc_own = idx_own % local
        flat = dev_own * capacity + slot_own

        x_rows, d_rows = [], []
        for l in range(local):
            d = jnp.einsum("ist,itd->isd", hot[:, l], dy_all, preferred_element_type=F32)
            d_rows.append((slot_gate[:, l, :, None] * d).astype(BF16).reshape(groups * capacity, -1))
        d_hid = [jnp.dot(d_rows[l], w_down[0, l].T, preferred_element_type=F32).astype(BF16) for l in range(local)]

        dx_back, o_rows, grads = [], [], []
        for l in range(local):
            x = jnp.einsum("ist,itd->isd", hot[:, l], x_all, preferred_element_type=F32).astype(BF16)
            x = x.reshape(groups * capacity, -1)
            a = jnp.dot(x, w_up[0, l], preferred_element_type=F32)
            b = jnp.dot(x, w_lin[0, l], preferred_element_type=F32)
            sig = jax.nn.sigmoid(a)
            act = a * sig
            hid = (act * b).astype(BF16)
            dh = d_hid[l].astype(F32)
            da = (dh * b * sig * (1.0 + a * (1.0 - sig))).astype(BF16)
            db = (dh * act).astype(BF16)
            dx = (jnp.dot(da, w_up[0, l].T, preferred_element_type=F32) + jnp.dot(db, w_lin[0, l].T, preferred_element_type=F32)).astype(BF16)
            dx_back.append(lax.all_to_all(dx.reshape(groups, capacity, -1), "expert", 0, 0, tiled=True))
            o_rows.append(jnp.dot(hid, w_down[0, l], preferred_element_type=F32).astype(BF16))
            grads.append((x, da, db, hid, d_rows[l]))
        o_back = [lax.all_to_all(o_rows[l].reshape(groups, capacity, -1), "expert", 0, 0, tiled=True) for l in range(local)]

        def wgrad(lhs, rhs):
            return jnp.einsum("rd,rf->df", lhs, rhs, preferred_element_type=F32).astype(BF16)

        g_up = jnp.stack([wgrad(g[0], g[1]) for g in grads])
        g_lin = jnp.stack([wgrad(g[0], g[2]) for g in grads])
        g_down = jnp.stack([wgrad(g[3], g[4]) for g in grads])

        cells = jnp.arange(groups * capacity, dtype=jnp.int32)
        dx_sum = jnp.zeros((), F32)
        y_sum = jnp.zeros((), F32)
        for l in range(local):
            at = jnp.where(loc_own == l, flat, -1)
            place = at[:, :, None] == cells[None, None, :]
            both = jnp.any(place, axis=0).astype(BF16)
            dx_sum = dx_sum + jnp.dot(both, dx_back[l].reshape(groups * capacity, -1), preferred_element_type=F32)
        dx_prev = lax.ppermute(dx_sum.astype(BF16), "stage", send_back)
        for l in range(local):
            at = jnp.where(loc_own == l, flat, -1)
            place = (at[:, :, None] == cells[None, None, :]).astype(BF16)
            copies = jnp.einsum("jtc,cd->jtd", place, o_back[l].reshape(groups * capacity, -1), preferred_element_type=F32)
            y_sum = y_sum + jnp.sum(gate_own[:, :, None] * copies, axis=0)
        return y_sum.astype(BF16)[None], dx_prev[None], g_up[None], g_lin[None], g_down[None]

    return jax.shard_map(device_step, mesh=mesh, in_specs=(tok_spec, tok_spec, tok_spec, w_spec, w_spec, w_spec, tok_spec), out_specs=(tok_spec, tok_spec, w_spec, w_spec, w_spec), check_vma=False)
```

```python
import functools

import jax
import jax.numpy as jnp
from jax import lax
from jax.experimental import pallas as pl
from jax.experimental.pallas import tpu as pltpu
from jax.sharding import PartitionSpec as P

F32 = jnp.float32
BF16 = jnp.bfloat16
ANY = pl.BlockSpec(memory_space=pl.ANY)
NT = (((1,), (1,)), ((), ()))
PARTS = 4


def earlier_counts(member):
    tokens = member.shape[-1]
    tok_ids = jnp.arange(tokens, dtype=jnp.int32)
    before = (tok_ids[:, None] < tok_ids[None, :]).astype(BF16)
    return jnp.dot(member.astype(BF16), before, preferred_element_type=F32).astype(jnp.int32)


def expert_kernel(stages, x_in, dy_in, meta_in, wu_in, wl_in, wd_in,
                  xb, dyb, xr, dr, hr, dar, dbr, dxr, orr,
                  wu, wl, wd, metab, posv, gatev, tri, oh, sg, stage_buf, dg, dh, xg, hb, dab, dbb, dxb, ob,
                  meta_s, meta_r, dy_s, dy_r, x_s, x_r, w_sem, load_sem, out_sem, dout_sem):
    tokens, width = x_in.shape
    cap = oh.shape[0] // 2
    ncol = 4
    cols = width // ncol
    rows = tokens // PARTS
    s = lax.axis_index("stage")
    e = lax.axis_index("expert")
    y, x, c = e // 4, (e // 2) % 2, e % 2
    s_next = (s + 1) % stages

    def peer(mask):
        py = 1 - y if mask & 4 else y
        px = 1 - x if mask & 2 else x
        pc = 1 - c if mask & 1 else c
        return py * 4 + px * 2 + pc

    def rcopy(src, dst, ssem, rsem, stage, mask):
        return pltpu.make_async_remote_copy(src_ref=src, dst_ref=dst, send_sem=ssem, recv_sem=rsem,
                                            device_id={"stage": stage, "expert": peer(mask)}, device_id_type=pl.DeviceIdType.MESH)

    sends = []

    def piece(ref, part):
        return ref.at[pl.ds(part * rows, rows)]

    def send(src, buf, slot, part, ssem, rsem, stage, mask):
        cp = rcopy(piece(src, part), piece(buf.at[slot], part), ssem.at[slot, part], rsem.at[slot, part], stage, mask)
        cp.start()
        sends.append(cp)

    def arrive(buf, slot, part, ssem, rsem):
        dst = piece(buf.at[slot], part)
        rcopy(dst, dst, ssem.at[slot, part], rsem.at[slot, part], s, 0).wait_recv()

    for m in range(8):
        cp = rcopy(meta_in, metab.at[m], meta_s.at[m], meta_r.at[m], s_next, m)
        cp.start()
        sends.append(cp)
    for part in range(PARTS):
        send(x_in, xb, 0, part, x_s, x_r, s_next, 0)
    for part in range(PARTS):
        for m in (2, 4, 1):
            send(dy_in, dyb, m, part, dy_s, dy_r, s, m)
    w_loads = [pltpu.make_async_copy(src, dst, w_sem.at[i]) for i, (src, dst) in enumerate(((wd_in, wd), (wu_in, wu), (wl_in, wl)))]
    for cp in w_loads:
        cp.start()

    def relay(buf, part, ssem, rsem):
        for m, other, own_half in ((2, 4, part < PARTS // 2), (4, 2, part >= PARTS // 2)):
            arrive(buf, m, part, ssem, rsem)
            send(buf.at[m], buf, m + 1, part, ssem, rsem, s, 1)
            if own_half:
                send(buf.at[m], buf, 6, part, ssem, rsem, s, other)

    def relay_diag(buf, part, ssem, rsem):
        arrive(buf, 6, part, ssem, rsem)
        send(buf.at[6], buf, 7, part, ssem, rsem, s, 1)

    t_row = lax.broadcasted_iota(jnp.int32, (tokens, tokens), 0)
    t_col = lax.broadcasted_iota(jnp.int32, (tokens, tokens), 1)
    tri[...] = (t_row < t_col).astype(F32).astype(BF16)
    for m in range(8):
        rcopy(meta_in, metab.at[m], meta_s.at[m], meta_r.at[m], s, 0).wait_recv()
    id0, id1, g0, g1 = (metab[:, k, :] for k in range(4))
    for l in range(2):
        mine = (e * 2 + l).astype(F32)
        in0, in1 = id0 == mine, id1 == mine
        gatev[pl.ds(l * 8, 8), :] = jnp.where(in0, g0, 0.0) + jnp.where(in1, g1, 0.0)
        posv[pl.ds(l * 8, 8), :] = jnp.where(in0 | in1, 1.0, 0.0)
    memb = posv[...]
    earlier = jnp.dot(memb.astype(BF16), tri[...], preferred_element_type=F32)
    posv[...] = jnp.where(memb > 0.5, earlier, -1.0)

    def one_hot(m, with_gate):
        slot = lax.broadcasted_iota(jnp.int32, (cap, tokens), 0).astype(F32)
        for l in range(2):
            hit = slot == posv[pl.ds(l * 8 + m, 1), :]
            oh[pl.ds(l * cap, cap), :] = jnp.where(hit, 1.0, 0.0).astype(BF16)
            if with_gate:
                sg[pl.ds(l * cap, cap), :] = jnp.sum(jnp.where(hit, gatev[pl.ds(l * 8 + m, 1), :], 0.0), axis=1, keepdims=True)

    def load(src, buf):
        return pltpu.make_async_copy(src, stage_buf.at[buf], load_sem.at[buf])

    def src_of(buf, own, m):
        return own if m == 0 and own is not None else buf.at[m]

    def row_of(rc):
        return pl.multiple_of((1 - c if rc else c) * cap, cap)

    def chip_of(g):
        return peer(2 * g) // 2

    def cotangent(g):
        for rc in range(2):
            load(src_of(dyb, dy_in, 2 * g + rc), rc).start()
        for rc in range(2):
            m = 2 * g + rc
            one_hot(m, True)
            load(src_of(dyb, dy_in, m), rc).wait()

            @pl.loop(0, ncol)
            def _(n):
                at = pl.ds(pl.multiple_of(n * cols, cols), cols)
                got = jnp.dot(oh[...], stage_buf[rc, :, at], preferred_element_type=F32)
                got = (sg[...] * got).astype(BF16)
                for l in range(2):
                    dg[l, g, pl.ds(row_of(rc), cap), at] = got[l * cap:(l + 1) * cap]

        @pl.loop(0, 2)
        def _(l):
            @pl.loop(0, ncol)
            def _(n):
                at = pl.ds(pl.multiple_of(n * cols, cols), cols)
                dh[l, g, :, at] = lax.dot_general(dg[l, g], wd[l, at, :], NT, preferred_element_type=F32).astype(BF16)
        for l in range(2):
            d_out(g, l).start()

    def d_out(g, l):
        return pltpu.make_async_copy(dg.at[l, g], dr.at[l, chip_of(g)], dout_sem.at[l, g])

    staged = ((xg, xr), (hb, hr), (dab, dar), (dbb, dbr), (dxb, dxr), (ob, orr))

    def outs(g, l):
        return [pltpu.make_async_copy(buf.at[l], out.at[l, chip_of(g)], out_sem.at[k, l]) for k, (buf, out) in enumerate(staged)]

    def expert_math(g):
        for rc in range(2):
            load(xb.at[2 * g + rc], rc).start()
        if g > 0:
            for l in range(2):
                for cp in outs(g - 1, l):
                    cp.wait()
        for rc in range(2):
            m = 2 * g + rc
            one_hot(m, False)
            load(xb.at[m], rc).wait()

            @pl.loop(0, ncol)
            def _(n):
                at = pl.ds(pl.multiple_of(n * cols, cols), cols)
                got = jnp.dot(oh[...], stage_buf[rc, :, at], preferred_element_type=F32).astype(BF16)
                for l in range(2):
                    xg[l, pl.ds(row_of(rc), cap), at] = got[l * cap:(l + 1) * cap]

        @pl.loop(0, 2)
        def _(l):
            @pl.loop(0, ncol)
            def _(n):
                at = pl.ds(pl.multiple_of(n * cols, cols), cols)
                a = jnp.dot(xg[l], wu[l, :, at], preferred_element_type=F32)
                b = jnp.dot(xg[l], wl[l, :, at], preferred_element_type=F32)
                sig = jax.nn.sigmoid(a)
                act = a * sig
                hb[l, :, at] = (act * b).astype(BF16)
                d_hid = dh[l, g, :, at].astype(F32)
                dab[l, :, at] = (d_hid * b * sig * (1.0 + a * (1.0 - sig))).astype(BF16)
                dbb[l, :, at] = (d_hid * act).astype(BF16)

            @pl.loop(0, ncol)
            def _(n):
                at = pl.ds(pl.multiple_of(n * cols, cols), cols)
                dxb[l, :, at] = (lax.dot_general(dab[l], wu[l, at, :], NT, preferred_element_type=F32)
                                 + lax.dot_general(dbb[l], wl[l, at, :], NT, preferred_element_type=F32)).astype(BF16)
                ob[l, :, at] = jnp.dot(hb[l], wd[l, :, at], preferred_element_type=F32).astype(BF16)
        for l in range(2):
            for cp in outs(g, l):
                cp.start()

    w_loads[0].wait()
    for part in range(PARTS):
        arrive(dyb, 1, part, dy_s, dy_r)
    cotangent(0)
    for part in range(PARTS):
        relay(dyb, part, dy_s, dy_r)
        arrive(xb, 0, part, x_s, x_r)
        for m in (2, 4, 1):
            send(xb.at[0], xb, m, part, x_s, x_r, s, m)
    for part in range(PARTS):
        arrive(xb, 1, part, x_s, x_r)
    w_loads[1].wait()
    w_loads[2].wait()
    expert_math(0)
    for part in range(PARTS):
        arrive(dyb, 3, part, dy_s, dy_r)
    cotangent(1)
    relay(xb, 0, x_s, x_r)
    for part in range(PARTS):
        arrive(dyb, 5, part, dy_s, dy_r)
    cotangent(2)
    for part in range(PARTS):
        relay_diag(dyb, part, dy_s, dy_r)
    relay(xb, 1, x_s, x_r)
    for part in range(PARTS):
        arrive(dyb, 7, part, dy_s, dy_r)
    cotangent(3)
    relay(xb, 2, x_s, x_r)
    relay(xb, 3, x_s, x_r)
    for part in range(PARTS):
        arrive(xb, 3, part, x_s, x_r)
    expert_math(1)
    relay_diag(xb, 0, x_s, x_r)
    relay_diag(xb, 2, x_s, x_r)
    for part in range(PARTS):
        arrive(xb, 5, part, x_s, x_r)
    expert_math(2)
    relay_diag(xb, 1, x_s, x_r)
    relay_diag(xb, 3, x_s, x_r)
    for part in range(PARTS):
        arrive(xb, 7, part, x_s, x_r)
    expert_math(3)
    for l in range(2):
        for cp in outs(3, l):
            cp.wait()
        for g in range(4):
            d_out(g, l).wait()
    for cp in sends:
        cp.wait_send()


def solution(mesh):
    stages = mesh.shape["stage"]
    groups = mesh.shape["expert"]
    send_next = [(src, (src + 1) % stages) for src in range(stages)]
    send_back = [(src, (src - 1) % stages) for src in range(stages)]
    tok_spec = P("stage", "expert", None)
    w_spec = P("stage", "expert", None, None)

    def device_step(x_act, route_idx, route_gate, w_up, w_lin, w_down, dy_out):
        tokens, width = x_act.shape[1:]
        local = w_up.shape[1]
        num_experts = local * groups
        capacity = 4 * tokens // num_experts

        meta = jnp.concatenate([route_idx[0].T.astype(F32), route_gate[0].T, jnp.zeros((4, tokens), F32)], axis=0)
        pair = 2 * capacity
        block = jax.ShapeDtypeStruct((8, tokens, width), BF16)
        rows_out = jax.ShapeDtypeStruct((local, 4, pair, width), BF16)
        outs = pl.pallas_call(
            functools.partial(expert_kernel, stages),
            out_shape=[block, block] + [rows_out] * 7,
            in_specs=[ANY] * 6,
            out_specs=[ANY] * 9,
            scratch_shapes=[
                pltpu.VMEM((local, width, width), BF16), pltpu.VMEM((local, width, width), BF16), pltpu.VMEM((local, width, width), BF16),
                pltpu.VMEM((8, 8, tokens), F32), pltpu.VMEM((16, tokens), F32), pltpu.VMEM((16, tokens), F32),
                pltpu.VMEM((tokens, tokens), BF16), pltpu.VMEM((pair, tokens), BF16), pltpu.VMEM((pair, 1), F32),
                pltpu.VMEM((2, tokens, width), BF16),
                pltpu.VMEM((local, 4, pair, width), BF16), pltpu.VMEM((local, 4, pair, width), BF16),
                *[pltpu.VMEM((local, pair, width), BF16) for _ in range(6)],
                pltpu.SemaphoreType.DMA((8,)), pltpu.SemaphoreType.DMA((8,)),
                pltpu.SemaphoreType.DMA((8, PARTS)), pltpu.SemaphoreType.DMA((8, PARTS)),
                pltpu.SemaphoreType.DMA((8, PARTS)), pltpu.SemaphoreType.DMA((8, PARTS)),
                pltpu.SemaphoreType.DMA((3,)), pltpu.SemaphoreType.DMA((2,)),
                pltpu.SemaphoreType.DMA((6, 2)), pltpu.SemaphoreType.DMA((2, 4)),
            ],
            compiler_params=pltpu.CompilerParams(has_side_effects=True, vmem_limit_bytes=62 * 1024 * 1024),
            name="expert_layer",
        )(x_act[0], dy_out[0], meta, w_up[0], w_lin[0], w_down[0])
        x_rows, d_rows, h_rows, da_rows, db_rows, dx_rows, o_rows = (o.reshape(local, groups * capacity, width) for o in outs[2:])

        def to_owners(rows):
            return lax.all_to_all(rows.reshape(groups, capacity, width), "expert", 0, 0, tiled=True).reshape(groups * capacity, width)

        dx_back = [to_owners(dx_rows[l]) for l in range(local)]
        o_back = [to_owners(o_rows[l]) for l in range(local)]

        def wgrad(lhs, rhs):
            return jnp.einsum("erd,erf->edf", lhs, rhs, preferred_element_type=F32).astype(BF16)

        g_up, g_lin, g_down = wgrad(x_rows, da_rows), wgrad(x_rows, db_rows), wgrad(h_rows, d_rows)

        meta = lax.ppermute(meta, "stage", send_next)
        idx_own = meta[:2].astype(jnp.int32)
        gate_own = meta[2:4]
        is_exp = idx_own[:, None, :] == jnp.arange(num_experts, dtype=jnp.int32)[None, :, None]
        pos_own = earlier_counts(jnp.any(is_exp, axis=0))
        slot_own = jnp.sum(jnp.where(is_exp, pos_own[None], 0), axis=1)
        loc_own = idx_own % local
        flat = idx_own // local * capacity + slot_own

        cells = jnp.arange(groups * capacity, dtype=jnp.int32)
        dx_sum = jnp.zeros((), F32)
        y_sum = jnp.zeros((), F32)
        for l in range(local):
            at = jnp.where(loc_own == l, flat, -1)
            both = jnp.any(at[:, :, None] == cells[None, None, :], axis=0).astype(BF16)
            dx_sum = dx_sum + jnp.dot(both, dx_back[l], preferred_element_type=F32)
        dx_prev = lax.ppermute(dx_sum.astype(BF16), "stage", send_back)
        for l in range(local):
            at = jnp.where(loc_own == l, flat, -1)
            place = (at[:, :, None] == cells[None, None, :]).astype(BF16)
            copies = jnp.einsum("jtc,cd->jtd", place, o_back[l], preferred_element_type=F32)
            y_sum = y_sum + jnp.sum(gate_own[:, :, None] * copies, axis=0)
        return y_sum.astype(BF16)[None], dx_prev[None], g_up[None], g_lin[None], g_down[None]

    return jax.shard_map(device_step, mesh=mesh, in_specs=(tok_spec, tok_spec, tok_spec, w_spec, w_spec, w_spec, tok_spec), out_specs=(tok_spec, tok_spec, w_spec, w_spec, w_spec), check_vma=False)
```

```python
import functools

import jax
import jax.numpy as jnp
from jax import lax
from jax.experimental import pallas as pl
from jax.experimental.pallas import tpu as pltpu
from jax.sharding import PartitionSpec as P

F32 = jnp.float32
BF16 = jnp.bfloat16
ANY = pl.BlockSpec(memory_space=pl.ANY)
NT = (((1,), (1,)), ((), ()))
TN = (((0,), (0,)), ((), ()))
PARTS = 4
NCOL = 4


def moe_kernel(stages, x_in, dy_in, meta_in, wu_in, wl_in, wd_in,
               y_out, dx_out, gu_out, gl_out, gd_out,
               xb, dyb, rdx, ro, xr, dr, hr, dar, dbr, dxr, orr, abr, dxs,
               wu, wl, wd, metab, posv, gatev, rowv, colv, tri, oh, sg, stage_buf, ab,
               xg, hb, ob, dgb, dhb, dab, dbb, dxb, ext, acc,
               meta_s, meta_r, dy_s, dy_r, x_s, x_r, rdx_s, rdx_r, ro_s, ro_r, z_s, z_r,
               w_sem, load_sem, f_sem, b_sem, ab_out, ab_in, g_load, g_out, misc_sem):
    tokens, width = x_in.shape
    cap = oh.shape[0] // 2
    pair = 2 * cap
    cols = width // NCOL
    rows = tokens // PARTS
    s = lax.axis_index("stage")
    e = lax.axis_index("expert")
    y, x, c = e // 4, (e // 2) % 2, e % 2
    s_next = (s + 1) % stages
    s_prev = (s + stages - 1) % stages

    def flip(mask):
        return 1 - y if mask & 4 else y, 1 - x if mask & 2 else x, 1 - c if mask & 1 else c

    def peer(mask):
        py, px, pc = flip(mask)
        return py * 4 + px * 2 + pc

    def rcopy(src, dst, ssem, rsem, stage, mask):
        return pltpu.make_async_remote_copy(src_ref=src, dst_ref=dst, send_sem=ssem, recv_sem=rsem,
                                            device_id={"stage": stage, "expert": peer(mask)}, device_id_type=pl.DeviceIdType.MESH)

    sends = []

    def push(src, dst, ssem, rsem, stage, mask):
        cp = rcopy(src, dst, ssem, rsem, stage, mask)
        cp.start()
        sends.append(cp)

    def landed(dst, rsem):
        rcopy(dst, dst, misc_sem.at[0], rsem, s, 0).wait_recv()

    def piece(ref, part):
        return ref.at[pl.ds(part * rows, rows)]

    def send(src, buf, slot, part, ssem, rsem, stage, mask):
        push(piece(src, part), piece(buf.at[slot], part), ssem.at[slot, part], rsem.at[slot, part], stage, mask)

    def arrive(buf, slot, part, rsem):
        landed(piece(buf.at[slot], part), rsem.at[slot, part])

    def arrive_all(buf, slot, rsem):
        for part in range(PARTS):
            arrive(buf, slot, part, rsem)

    def relay(buf, part, ssem, rsem):
        for m, other, own_half in ((2, 4, part < PARTS // 2), (4, 2, part >= PARTS // 2)):
            arrive(buf, m, part, rsem)
            if own_half:
                send(buf.at[m], buf, 6, part, ssem, rsem, s, other)
            send(buf.at[m], buf, m + 1, part, ssem, rsem, s, 1)

    def relay_diag(buf, part, ssem, rsem):
        arrive(buf, 6, part, rsem)
        send(buf.at[6], buf, 7, part, ssem, rsem, s, 1)

    def col(n):
        return pl.ds(pl.multiple_of(n * cols, cols), cols)

    def row_of(rc):
        return pl.multiple_of((1 - c if rc else c) * cap, cap)

    def own_rows(ref, l, g, rc):
        py, px, _ = flip(2 * g)
        return ref.at[l, py * 2 + px, pl.ds(row_of(rc), cap)]

    def chip_rows(ref, l, g):
        py, px, _ = flip(2 * g)
        if ref.shape[1] == 4:
            return ref.at[l, py * 2 + px]
        return ref.at[l, py, pl.ds(pl.multiple_of(px * pair, pair), pair)]

    for m in range(8):
        push(meta_in, metab.at[m], meta_s.at[m], meta_r.at[m], s_next, m)
    for part in range(PARTS):
        send(x_in, xb, 0, part, x_s, x_r, s_next, 0)
    for part in range(PARTS):
        for m in (2, 4, 1) if part == 0 else (1,):
            send(dy_in, dyb, m, part, dy_s, dy_r, s, m)
    w_loads = [pltpu.make_async_copy(src, dst, w_sem.at[i]) for i, (src, dst) in enumerate(((wu_in, wu), (wl_in, wl), (wd_in, wd)))]
    for cp in w_loads:
        cp.start()

    t_row = lax.broadcasted_iota(jnp.int32, (tokens, tokens), 0)
    t_col = lax.broadcasted_iota(jnp.int32, (tokens, tokens), 1)
    tri[...] = (t_row < t_col).astype(F32).astype(BF16)
    for m in range(8):
        landed(metab.at[m], meta_r.at[m])
    id0, id1, g0, g1 = (metab[:, k, :] for k in range(4))
    for l in range(2):
        mine = (e * 2 + l).astype(F32)
        in0, in1 = id0 == mine, id1 == mine
        gatev[pl.ds(l * 8, 8), :] = jnp.where(in0, g0, 0.0) + jnp.where(in1, g1, 0.0)
        posv[pl.ds(l * 8, 8), :] = jnp.where(in0 | in1, 1.0, 0.0)
    memb = posv[...]
    earlier = jnp.dot(memb.astype(BF16), tri[...], preferred_element_type=F32)
    posv[...] = jnp.where(memb > 0.5, earlier, -1.0)

    def owner_routing():
        rowv[...] = jnp.zeros_like(rowv)
        o0, o1 = metab[0, 0:1, :], metab[0, 1:2, :]
        experts = [(peer(m) * 2 + l).astype(F32) for m in range(8) for l in range(2)]
        for r, mine in enumerate(experts):
            rowv[pl.ds(r, 1), :] = jnp.where((o0 == mine) | (o1 == mine), 1.0, 0.0)
        before = jnp.dot(rowv[pl.ds(0, 16), :].astype(BF16), tri[...], preferred_element_type=F32)
        for r, mine in enumerate(experts):
            rowv[pl.ds(r, 1), :] = jnp.where(o0 == mine, before[r:r + 1], -1.0)
            rowv[pl.ds(16 + r, 1), :] = jnp.where(o1 == mine, before[r:r + 1], -1.0)
        rowv[pl.ds(32, 2), :] = metab[0, 2:4, :]
        colv[...] = rowv[...].T

    def one_hot(m, with_gate):
        slot = lax.broadcasted_iota(jnp.int32, (cap, tokens), 0).astype(F32)
        for l in range(2):
            hit = slot == posv[pl.ds(l * 8 + m, 1), :]
            oh[pl.ds(l * cap, cap), :] = jnp.where(hit, 1.0, 0.0).astype(BF16)
            if with_gate:
                sg[pl.ds(l * cap, cap), :] = jnp.sum(jnp.where(hit, gatev[pl.ds(l * 8 + m, 1), :], 0.0), axis=1, keepdims=True)

    def load(src, buf):
        return pltpu.make_async_copy(src, stage_buf.at[buf], load_sem.at[buf])

    def gather(buf, own, g, into, with_gate):
        srcs = [own if (2 * g + rc == 0 and own is not None) else buf.at[2 * g + rc] for rc in range(2)]
        for rc in range(2):
            load(srcs[rc], rc).start()
        for rc in range(2):
            one_hot(2 * g + rc, with_gate)
            load(srcs[rc], rc).wait()

            @pl.loop(0, NCOL)
            def _(n):
                at = col(n)
                got = jnp.dot(oh[...], stage_buf[rc, :, at], preferred_element_type=F32)
                if with_gate:
                    got = sg[...] * got
                got = got.astype(BF16)
                for l in range(2):
                    into[l, pl.ds(row_of(rc), cap), at] = got[l * cap:(l + 1) * cap]

    def f_outs(g, l):
        return [pltpu.make_async_copy(buf.at[l], chip_rows(out, l, g), f_sem.at[k, l]) for k, (buf, out) in enumerate(((xg, xr), (hb, hr), (ob, orr)))]

    def b_outs(g, l):
        return [pltpu.make_async_copy(buf.at[l], chip_rows(out, l, g), b_sem.at[k, l]) for k, (buf, out) in enumerate(((dgb, dr), (dab, dar), (dbb, dbr), (dxb, dxr)))]

    def ab_store(g, l):
        return pltpu.make_async_copy(ab.at[l], abr.at[l, g], ab_out.at[l])

    def ab_load(g, l):
        return pltpu.make_async_copy(abr.at[l, g], ab.at[l], ab_in.at[l])

    def wait_f(g):
        for l in range(2):
            for cp in f_outs(g, l):
                cp.wait()
            ab_store(g, l).wait()

    def forward(g):
        if g > 0:
            wait_f(g - 1)
        gather(xb, None, g, xg, False)
        for l in range(2):
            @pl.loop(0, NCOL)
            def _(n):
                at = col(n)
                a = jnp.dot(xg[l], wu[l, :, at], preferred_element_type=F32)
                b = jnp.dot(xg[l], wl[l, :, at], preferred_element_type=F32)
                ab[l, 0, :, at] = a
                ab[l, 1, :, at] = b
                hb[l, :, at] = (a * jax.nn.sigmoid(a) * b).astype(BF16)
            ab_store(g, l).start()

            @pl.loop(0, NCOL)
            def _(n):
                at = col(n)
                ob[l, :, at] = jnp.dot(hb[l], wd[l, :, at], preferred_element_type=F32).astype(BF16)
            for cp in f_outs(g, l):
                cp.start()

    def send_back(rows_ref, into, g, ssem, rsem):
        for l in range(2):
            for rc in range(2):
                m = 2 * g + rc
                if m:
                    push(own_rows(rows_ref, l, g, rc), into.at[m, pl.ds(l * cap, cap)], ssem.at[m, l], rsem.at[m, l], s, m)

    def backward(g):
        if g == 0:
            for l in range(2):
                ab_load(0, l).start()
        else:
            for l in range(2):
                for cp in b_outs(g - 1, l)[:3]:
                    cp.wait()
        gather(dyb, dy_in, g, dgb, True)
        for l in range(2):
            ab_load(g, l).wait()

            @pl.loop(0, NCOL)
            def _(n):
                at = col(n)
                dhb[...] = lax.dot_general(dgb[l], wd[l, at, :], NT, preferred_element_type=F32).astype(BF16)
                d_hid = dhb[...].astype(F32)
                a, b = ab[l, 0, :, at], ab[l, 1, :, at]
                sig = jax.nn.sigmoid(a)
                dab[l, :, at] = (d_hid * b * sig * (1.0 + a * (1.0 - sig))).astype(BF16)
                dbb[l, :, at] = (d_hid * (a * sig)).astype(BF16)
            if g < 3:
                ab_load(g + 1, l).start()

            @pl.loop(0, NCOL)
            def _(n):
                at = col(n)
                dxb[l, :, at] = (lax.dot_general(dab[l], wu[l, at, :], NT, preferred_element_type=F32)
                                 + lax.dot_general(dbb[l], wl[l, at, :], NT, preferred_element_type=F32)).astype(BF16)
            for cp in b_outs(g, l):
                cp.start()
        for l in range(2):
            b_outs(g, l)[3].wait()
        send_back(dxr, rdx, g, rdx_s, rdx_r)

    for part in range(PARTS):
        arrive(xb, 0, part, x_r)
        for m in (2, 4, 1):
            send(xb.at[0], xb, m, part, x_s, x_r, s, m)
        if part > 0:
            relay(xb, part - 1, x_s, x_r)
    for m in (2, 4):
        send(dy_in, dyb, m, 1, dy_s, dy_r, s, m)
    owner_routing()
    for cp in w_loads:
        cp.wait()
    relay(xb, PARTS - 1, x_s, x_r)
    for part in (2, 3):
        for m in (2, 4):
            send(dy_in, dyb, m, part, dy_s, dy_r, s, m)
    arrive_all(xb, 1, x_r)
    forward(0)
    relay_diag(xb, 0, x_s, x_r)
    relay_diag(xb, 2, x_s, x_r)
    relay(dyb, 0, dy_s, dy_r)
    arrive_all(xb, 3, x_r)
    forward(1)
    relay_diag(xb, 1, x_s, x_r)
    relay_diag(xb, 3, x_s, x_r)
    arrive_all(xb, 5, x_r)
    forward(2)
    relay(dyb, 1, dy_s, dy_r)
    arrive_all(xb, 7, x_r)
    forward(3)
    relay(dyb, 2, dy_s, dy_r)
    wait_f(3)
    arrive_all(dyb, 1, dy_r)
    backward(0)
    relay(dyb, 3, dy_s, dy_r)
    arrive_all(dyb, 3, dy_r)
    backward(1)
    relay_diag(dyb, 0, dy_s, dy_r)
    relay_diag(dyb, 1, dy_s, dy_r)
    arrive_all(dyb, 5, dy_r)
    backward(2)
    relay_diag(dyb, 2, dy_s, dy_r)
    relay_diag(dyb, 3, dy_s, dy_r)
    arrive_all(dyb, 7, dy_r)
    backward(3)
    for g in (1, 2, 3, 0):
        send_back(orr, ro, g, ro_s, ro_r)
    for l in range(2):
        for cp in b_outs(3, l)[:3]:
            cp.wait()

    def g_copies(l):
        bufs = (xg, hb, ob) if l == 0 else (dgb, dab, dbb)
        return [pltpu.make_async_copy(buf.at[half], out.at[l, pl.ds(half * pair, pair)], g_out.at[l, k, half])
                for k, (buf, out) in enumerate(zip(bufs, (gu_out, gl_out, gd_out))) for half in range(2)]

    def weight_grads(l):
        loads = [pltpu.make_async_copy(src.at[l], dst, g_load.at[k]) for k, (src, dst) in enumerate(((xr, wu), (dar, ext.at[0]), (dbr, ext.at[1]), (hr, wl), (dr, wd)))]
        for cp in loads:
            cp.start()
        bufs = (xg, hb, ob) if l == 0 else (dgb, dab, dbb)
        block = pair // 2
        for k, (lhs, rhs, need) in enumerate(((wu, ext.at[0], loads[:2]), (wu, ext.at[1], loads[2:3]), (wl, wd, loads[3:]))):
            for cp in need:
                cp.wait()

            @pl.loop(0, width // block)
            def _(i):
                at = pl.ds(pl.multiple_of(i * block, block), block)
                total = (lax.dot_general(lhs[0, :, at], rhs[0], TN, preferred_element_type=F32)
                         + lax.dot_general(lhs[1, :, at], rhs[1], TN, preferred_element_type=F32))
                bufs[k][i // 2, pl.ds(pl.multiple_of(i % 2 * block, block), block), :] = total.astype(BF16)
        for cp in g_copies(l):
            cp.start()

    def returned(rows_ref, into, g, rsem):
        b = g % 2
        for m in (2 * g, 2 * g + 1):
            if m:
                for l in range(2):
                    landed(into.at[m, pl.ds(l * cap, cap)], rsem.at[m, l])
        copies = []
        for rc in range(2):
            m = 2 * g + rc
            for l in range(2):
                src = into.at[m, pl.ds(l * cap, cap)] if m else own_rows(rows_ref, l, 0, 0)
                copies.append(pltpu.make_async_copy(src, stage_buf.at[b, pl.ds((rc * 2 + l) * cap, cap)], misc_sem.at[1 + rc * 2 + l]))
        for cp in copies:
            cp.start()
        for cp in copies:
            cp.wait()
        return b

    def place(into, g, which):
        slot = lax.broadcasted_iota(jnp.int32, (tokens, cap), 1).astype(F32)
        for k in range(4):
            r = 4 * g + k
            at0, at1 = colv[:, r:r + 1], colv[:, 16 + r:17 + r]
            at = (at0, at1, jnp.maximum(at0, at1))[which]
            into[:, pl.ds(k * cap, cap)] = jnp.where(slot == at, 1.0, 0.0).astype(BF16)

    def combine_dx(g):
        place(tri, g, 2)
        b = returned(dxr, rdx, g, rdx_r)

        @pl.loop(0, NCOL)
        def _(n):
            at = col(n)
            got = jnp.dot(tri[...], stage_buf[b, :, at], preferred_element_type=F32)
            if g > 0:
                got = acc[0, :, at] + got
            if g < 3:
                acc[0, :, at] = got
            else:
                stage_buf[1 - b, :, at] = got.astype(BF16)
        if g == 3:
            cp = pltpu.make_async_copy(stage_buf.at[1 - b], dxs, misc_sem.at[1])
            cp.start()
            cp.wait()
            for part in range(PARTS):
                push(piece(dxs, part), piece(dx_out, part), z_s.at[part], z_r.at[part], s_prev, 0)

    def combine_y(g):
        for j in range(2):
            place(ext.at[0, j], g, j)
        b = returned(orr, ro, g, ro_r)

        @pl.loop(0, NCOL)
        def _(n):
            at = col(n)
            got = [jnp.dot(ext[0, j], stage_buf[b, :, at], preferred_element_type=F32) for j in range(2)]
            if g > 0:
                got = [acc[j, :, at] + got[j] for j in range(2)]
            if g < 3:
                for j in range(2):
                    acc[j, :, at] = got[j]
            else:
                stage_buf[1 - b, :, at] = (colv[:, 32:33] * got[0] + colv[:, 33:34] * got[1]).astype(BF16)
        if g == 3:
            cp = pltpu.make_async_copy(stage_buf.at[1 - b], y_out, misc_sem.at[1])
            cp.start()
            cp.wait()

    weight_grads(0)
    combine_dx(0)
    combine_dx(1)
    combine_dx(2)
    combine_dx(3)
    weight_grads(1)
    for g in range(4):
        combine_y(g)
    for l in range(2):
        for cp in g_copies(l):
            cp.wait()
    for part in range(PARTS):
        landed(piece(dx_out, part), z_r.at[part])
    for cp in sends:
        cp.wait_send()


def solution(mesh):
    stages = mesh.shape["stage"]
    groups = mesh.shape["expert"]
    tok_spec = P("stage", "expert", None)
    w_spec = P("stage", "expert", None, None)

    def device_step(x_act, route_idx, route_gate, w_up, w_lin, w_down, dy_out):
        tokens, width = x_act.shape[1:]
        local = w_up.shape[1]
        cap = 4 * tokens // (local * groups)
        pair = 2 * cap
        meta = jnp.concatenate([route_idx[0].T.astype(F32), route_gate[0].T, jnp.zeros((4, tokens), F32)], axis=0)

        def arr(*shape, dtype=BF16):
            return jax.ShapeDtypeStruct(shape, dtype)

        def dma(*shape):
            return pltpu.SemaphoreType.DMA(shape)

        tok, weight = arr(tokens, width), arr(local, width, width)
        by_half, by_chip = arr(local, 2, 2 * pair, width), arr(local, 4, pair, width)
        vm = pltpu.VMEM
        outs = pl.pallas_call(
            functools.partial(moe_kernel, stages),
            out_shape=[tok, tok, weight, weight, weight,
                       arr(8, tokens, width), arr(8, tokens, width), arr(8, pair, width), arr(8, pair, width),
                       *[by_half] * 5, by_chip, by_chip, arr(local, 4, 2, pair, width, dtype=F32), tok],
            in_specs=[ANY] * 6,
            out_specs=[ANY] * 18,
            scratch_shapes=[
                *[vm((local, width, width), BF16)] * 3,
                vm((8, 8, tokens), F32), vm((16, tokens), F32), vm((16, tokens), F32), vm((128, tokens), F32), vm((tokens, 128), F32),
                vm((tokens, tokens), BF16), vm((pair, tokens), BF16), vm((pair, 1), F32),
                vm((2, tokens, width), BF16), vm((local, 2, pair, width), F32),
                *[vm((local, pair, width), BF16)] * 4, vm((pair, width // NCOL), BF16), *[vm((local, pair, width), BF16)] * 3,
                vm((2, 2, tokens, width), BF16), vm((2, tokens, width), F32),
                dma(8), dma(8), dma(8, PARTS), dma(8, PARTS), dma(8, PARTS), dma(8, PARTS),
                dma(8, 2), dma(8, 2), dma(8, 2), dma(8, 2), dma(PARTS), dma(PARTS),
                dma(3), dma(2), dma(3, 2), dma(4, 2), dma(2), dma(2), dma(5), dma(2, 3, 2), dma(5),
            ],
            compiler_params=pltpu.CompilerParams(has_side_effects=True, vmem_limit_bytes=63 * 1024 * 1024),
            name="moe_layer",
        )(x_act[0], dy_out[0], meta, w_up[0], w_lin[0], w_down[0])
        return tuple(o[None] for o in outs[:5])

    return jax.shard_map(device_step, mesh=mesh, in_specs=(tok_spec, tok_spec, tok_spec, w_spec, w_spec, w_spec, tok_spec), out_specs=(tok_spec, tok_spec, w_spec, w_spec, w_spec), check_vma=False)
```

```python
import functools

import jax
import jax.numpy as jnp
from jax import lax
from jax.experimental import pallas as pl
from jax.experimental.pallas import tpu as pltpu
from jax.sharding import PartitionSpec as P

F32 = jnp.float32
BF16 = jnp.bfloat16
ANY = pl.BlockSpec(memory_space=pl.ANY)
NT = (((1,), (1,)), ((), ()))
TN = (((0,), (0,)), ((), ()))
PARTS = 4
NCOL = 4


def moe_kernel(stages, x_in, dy_in, meta_in, wu_in, wl_in, wd_in,
               y_out, dx_out, gu_out, gl_out, gd_out,
               xb, dyb, rdx, ro, xr, dr, hr, dar, dbr, dxr, orr, abr, dxs,
               wu, wl, wd, metab, posv, gatev, rowv, colv, tri, oh, sg, stage_buf, ab,
               xg, hb, ob, dgb, dhb, dab, dbb, dxb, ext, acc,
               meta_s, meta_r, dy_s, dy_r, x_s, x_r, rdx_s, rdx_r, ro_s, ro_r, z_s, z_r,
               w_sem, load_sem, f_sem, b_sem, ab_out, ab_in, g_load, g_out, misc_sem):
    tokens, width = x_in.shape
    cap = oh.shape[0] // 2
    pair = 2 * cap
    cols = width // NCOL
    rows = tokens // PARTS
    s = lax.axis_index("stage")
    e = lax.axis_index("expert")
    y, x, c = e // 4, (e // 2) % 2, e % 2
    s_next = (s + 1) % stages
    s_prev = (s + stages - 1) % stages

    def flip(mask):
        return 1 - y if mask & 4 else y, 1 - x if mask & 2 else x, 1 - c if mask & 1 else c

    def peer(mask):
        py, px, pc = flip(mask)
        return py * 4 + px * 2 + pc

    def rcopy(src, dst, ssem, rsem, stage, mask):
        return pltpu.make_async_remote_copy(src_ref=src, dst_ref=dst, send_sem=ssem, recv_sem=rsem,
                                            device_id={"stage": stage, "expert": peer(mask)}, device_id_type=pl.DeviceIdType.MESH)

    sends = []

    def push(src, dst, ssem, rsem, stage, mask):
        cp = rcopy(src, dst, ssem, rsem, stage, mask)
        cp.start()
        sends.append(cp)

    def landed(dst, rsem):
        rcopy(dst, dst, misc_sem.at[0], rsem, s, 0).wait_recv()

    def piece(ref, part):
        return ref.at[pl.ds(part * rows, rows)]

    def send(src, buf, slot, part, ssem, rsem, stage, mask):
        push(piece(src, part), piece(buf.at[slot], part), ssem.at[slot, part], rsem.at[slot, part], stage, mask)

    def arrive(buf, slot, part, rsem):
        landed(piece(buf.at[slot], part), rsem.at[slot, part])

    def arrive_all(buf, slot, rsem):
        for part in range(PARTS):
            arrive(buf, slot, part, rsem)

    def relay(buf, part, ssem, rsem):
        for m, other, own_half in ((2, 4, part < PARTS // 2), (4, 2, part >= PARTS // 2)):
            arrive(buf, m, part, rsem)
            if own_half:
                send(buf.at[m], buf, 6, part, ssem, rsem, s, other)
            send(buf.at[m], buf, m + 1, part, ssem, rsem, s, 1)

    def relay_diag(buf, part, ssem, rsem):
        arrive(buf, 6, part, rsem)
        send(buf.at[6], buf, 7, part, ssem, rsem, s, 1)

    def col(n):
        return pl.ds(pl.multiple_of(n * cols, cols), cols)

    def row_of(rc):
        return pl.multiple_of((1 - c if rc else c) * cap, cap)

    def own_rows(ref, l, g, rc):
        py, px, _ = flip(2 * g)
        return ref.at[l, py * 2 + px, pl.ds(row_of(rc), cap)]

    def chip_rows(ref, l, g):
        py, px, _ = flip(2 * g)
        if ref.shape[1] == 4:
            return ref.at[l, py * 2 + px]
        return ref.at[l, py, pl.ds(pl.multiple_of(px * pair, pair), pair)]

    for m in range(8):
        push(meta_in, metab.at[m], meta_s.at[m], meta_r.at[m], s_next, m)
    def send_z(part):
        send(x_in, xb, 0, part, x_s, x_r, s_next, 0)

    send_z(0)
    for m in (2, 4):
        send(dy_in, dyb, m, 0, dy_s, dy_r, s, m)
    send_z(1)
    for part in range(PARTS):
        send(dy_in, dyb, 1, part, dy_s, dy_r, s, 1)
    w_loads = [pltpu.make_async_copy(src, dst, w_sem.at[i]) for i, (src, dst) in enumerate(((wu_in, wu), (wl_in, wl), (wd_in, wd)))]
    for cp in w_loads:
        cp.start()

    t_row = lax.broadcasted_iota(jnp.int32, (tokens, tokens), 0)
    t_col = lax.broadcasted_iota(jnp.int32, (tokens, tokens), 1)
    tri[...] = (t_row < t_col).astype(F32).astype(BF16)
    for m in range(8):
        landed(metab.at[m], meta_r.at[m])
    id0, id1, g0, g1 = (metab[:, k, :] for k in range(4))
    for l in range(2):
        mine = (e * 2 + l).astype(F32)
        in0, in1 = id0 == mine, id1 == mine
        gatev[pl.ds(l * 8, 8), :] = jnp.where(in0, g0, 0.0) + jnp.where(in1, g1, 0.0)
        posv[pl.ds(l * 8, 8), :] = jnp.where(in0 | in1, 1.0, 0.0)
    memb = posv[...]
    earlier = jnp.dot(memb.astype(BF16), tri[...], preferred_element_type=F32)
    posv[...] = jnp.where(memb > 0.5, earlier, -1.0)

    def owner_routing():
        rowv[...] = jnp.zeros_like(rowv)
        o0, o1 = metab[0, 0:1, :], metab[0, 1:2, :]
        experts = [(peer(m) * 2 + l).astype(F32) for m in range(8) for l in range(2)]
        for r, mine in enumerate(experts):
            rowv[pl.ds(r, 1), :] = jnp.where((o0 == mine) | (o1 == mine), 1.0, 0.0)
        before = jnp.dot(rowv[pl.ds(0, 16), :].astype(BF16), tri[...], preferred_element_type=F32)
        for r, mine in enumerate(experts):
            rowv[pl.ds(r, 1), :] = jnp.where(o0 == mine, before[r:r + 1], -1.0)
            rowv[pl.ds(16 + r, 1), :] = jnp.where(o1 == mine, before[r:r + 1], -1.0)
        rowv[pl.ds(32, 2), :] = metab[0, 2:4, :]
        colv[...] = rowv[...].T

    def one_hot(m, with_gate):
        slot = lax.broadcasted_iota(jnp.int32, (cap, tokens), 0).astype(F32)
        for l in range(2):
            hit = slot == posv[pl.ds(l * 8 + m, 1), :]
            oh[pl.ds(l * cap, cap), :] = jnp.where(hit, 1.0, 0.0).astype(BF16)
            if with_gate:
                sg[pl.ds(l * cap, cap), :] = jnp.sum(jnp.where(hit, gatev[pl.ds(l * 8 + m, 1), :], 0.0), axis=1, keepdims=True)

    def load(src, buf):
        return pltpu.make_async_copy(src, stage_buf.at[buf], load_sem.at[buf])

    def gather(buf, own, g, into, with_gate):
        srcs = [own if (2 * g + rc == 0 and own is not None) else buf.at[2 * g + rc] for rc in range(2)]
        for rc in range(2):
            load(srcs[rc], rc).start()
        for rc in range(2):
            one_hot(2 * g + rc, with_gate)
            load(srcs[rc], rc).wait()

            @pl.loop(0, NCOL)
            def _(n):
                at = col(n)
                got = jnp.dot(oh[...], stage_buf[rc, :, at], preferred_element_type=F32)
                if with_gate:
                    got = sg[...] * got
                got = got.astype(BF16)
                for l in range(2):
                    into[l, pl.ds(row_of(rc), cap), at] = got[l * cap:(l + 1) * cap]

    def f_outs(g, l):
        return [pltpu.make_async_copy(buf.at[l], chip_rows(out, l, g), f_sem.at[k, l]) for k, (buf, out) in enumerate(((xg, xr), (hb, hr), (ob, orr)))]

    def b_outs(g, l):
        return [pltpu.make_async_copy(buf.at[l], chip_rows(out, l, g), b_sem.at[k, l]) for k, (buf, out) in enumerate(((dgb, dr), (dab, dar), (dbb, dbr), (dxb, dxr)))]

    def ab_store(g, l):
        return pltpu.make_async_copy(ab.at[l], abr.at[l, g], ab_out.at[l])

    def ab_load(g, l):
        return pltpu.make_async_copy(abr.at[l, g], ab.at[l], ab_in.at[l])

    def wait_f(g):
        for l in range(2):
            for cp in f_outs(g, l):
                cp.wait()
            ab_store(g, l).wait()

    def forward(g):
        if g > 0:
            wait_f(g - 1)
        gather(xb, None, g, xg, False)
        for l in range(2):
            @pl.loop(0, NCOL)
            def _(n):
                at = col(n)
                a = jnp.dot(xg[l], wu[l, :, at], preferred_element_type=F32)
                b = jnp.dot(xg[l], wl[l, :, at], preferred_element_type=F32)
                ab[l, 0, :, at] = a
                ab[l, 1, :, at] = b
                hb[l, :, at] = (a * jax.nn.sigmoid(a) * b).astype(BF16)
            ab_store(g, l).start()

            @pl.loop(0, NCOL)
            def _(n):
                at = col(n)
                ob[l, :, at] = jnp.dot(hb[l], wd[l, :, at], preferred_element_type=F32).astype(BF16)
            for cp in f_outs(g, l):
                cp.start()

    def send_back(rows_ref, into, chips, ssem, rsem):
        for l in range(2):
            for m, g, rc in ((2 * g + rc, g, rc) for rc in range(2) for g in chips):
                if m:
                    push(own_rows(rows_ref, l, g, rc), into.at[m, pl.ds(l * cap, cap)], ssem.at[m, l], rsem.at[m, l], s, m)

    def backward(g):
        if g == 0:
            for l in range(2):
                ab_load(0, l).start()
        else:
            for l in range(2):
                for cp in b_outs(g - 1, l)[:3]:
                    cp.wait()
        gather(dyb, dy_in, g, dgb, True)
        for l in range(2):
            ab_load(g, l).wait()

            @pl.loop(0, NCOL)
            def _(n):
                at = col(n)
                dhb[...] = lax.dot_general(dgb[l], wd[l, at, :], NT, preferred_element_type=F32).astype(BF16)
                d_hid = dhb[...].astype(F32)
                a, b = ab[l, 0, :, at], ab[l, 1, :, at]
                sig = jax.nn.sigmoid(a)
                dab[l, :, at] = (d_hid * b * sig * (1.0 + a * (1.0 - sig))).astype(BF16)
                dbb[l, :, at] = (d_hid * (a * sig)).astype(BF16)
            if g < 3:
                ab_load(g + 1, l).start()

            @pl.loop(0, NCOL)
            def _(n):
                at = col(n)
                dxb[l, :, at] = (lax.dot_general(dab[l], wu[l, at, :], NT, preferred_element_type=F32)
                                 + lax.dot_general(dbb[l], wl[l, at, :], NT, preferred_element_type=F32)).astype(BF16)
            for cp in b_outs(g, l):
                cp.start()
        for l in range(2):
            b_outs(g, l)[3].wait()
        for chips in ((0,), (), (1, 2), (3,))[g:g + 1]:
            send_back(dxr, rdx, chips, rdx_s, rdx_r)

    for part in range(PARTS):
        arrive(xb, 0, part, x_r)
        if part + 2 < PARTS:
            send_z(part + 2)
        for m in (2, 4, 1):
            send(xb.at[0], xb, m, part, x_s, x_r, s, m)
        if part > 0:
            relay(xb, part - 1, x_s, x_r)
    for m in (2, 4):
        send(dy_in, dyb, m, 1, dy_s, dy_r, s, m)
    owner_routing()
    for cp in w_loads:
        cp.wait()
    relay(xb, PARTS - 1, x_s, x_r)
    for part in (2, 3):
        for m in (2, 4):
            send(dy_in, dyb, m, part, dy_s, dy_r, s, m)
    arrive_all(xb, 1, x_r)
    forward(0)
    relay_diag(xb, 0, x_s, x_r)
    relay_diag(xb, 2, x_s, x_r)
    relay(dyb, 0, dy_s, dy_r)
    arrive_all(xb, 3, x_r)
    forward(1)
    relay_diag(xb, 1, x_s, x_r)
    relay_diag(xb, 3, x_s, x_r)
    arrive_all(xb, 5, x_r)
    forward(2)
    relay(dyb, 1, dy_s, dy_r)
    arrive_all(xb, 7, x_r)
    forward(3)
    relay(dyb, 2, dy_s, dy_r)
    wait_f(3)
    arrive_all(dyb, 1, dy_r)
    backward(0)
    relay(dyb, 3, dy_s, dy_r)
    arrive_all(dyb, 3, dy_r)
    backward(1)
    relay_diag(dyb, 0, dy_s, dy_r)
    relay_diag(dyb, 1, dy_s, dy_r)
    arrive_all(dyb, 5, dy_r)
    backward(2)
    relay_diag(dyb, 2, dy_s, dy_r)
    relay_diag(dyb, 3, dy_s, dy_r)
    arrive_all(dyb, 7, dy_r)
    backward(3)
    for chips in ((0,), (1, 2), (3,)):
        send_back(orr, ro, chips, ro_s, ro_r)
    for l in range(2):
        for cp in b_outs(3, l)[:3]:
            cp.wait()

    def g_copies(l):
        bufs = (xg, hb, ob) if l == 0 else (dgb, dab, dbb)
        return [pltpu.make_async_copy(buf.at[half], out.at[l, pl.ds(half * pair, pair)], g_out.at[l, k, half])
                for k, (buf, out) in enumerate(zip(bufs, (gu_out, gl_out, gd_out))) for half in range(2)]

    def weight_grads(l):
        loads = [pltpu.make_async_copy(src.at[l], dst, g_load.at[k]) for k, (src, dst) in enumerate(((xr, wu), (dar, ext.at[0]), (dbr, ext.at[1]), (hr, wl), (dr, wd)))]
        for cp in loads:
            cp.start()
        bufs = (xg, hb, ob) if l == 0 else (dgb, dab, dbb)
        block = pair // 2
        for k, (lhs, rhs, need) in enumerate(((wu, ext.at[0], loads[:2]), (wu, ext.at[1], loads[2:3]), (wl, wd, loads[3:]))):
            for cp in need:
                cp.wait()

            @pl.loop(0, width // block)
            def _(i):
                at = pl.ds(pl.multiple_of(i * block, block), block)
                total = (lax.dot_general(lhs[0, :, at], rhs[0], TN, preferred_element_type=F32)
                         + lax.dot_general(lhs[1, :, at], rhs[1], TN, preferred_element_type=F32))
                bufs[k][i // 2, pl.ds(pl.multiple_of(i % 2 * block, block), block), :] = total.astype(BF16)
        for cp in g_copies(l):
            cp.start()

    def returned(rows_ref, into, g, rsem):
        b = g % 2
        for m in (2 * g, 2 * g + 1):
            if m:
                for l in range(2):
                    landed(into.at[m, pl.ds(l * cap, cap)], rsem.at[m, l])
        copies = []
        for rc in range(2):
            m = 2 * g + rc
            for l in range(2):
                src = into.at[m, pl.ds(l * cap, cap)] if m else own_rows(rows_ref, l, 0, 0)
                copies.append(pltpu.make_async_copy(src, stage_buf.at[b, pl.ds((rc * 2 + l) * cap, cap)], misc_sem.at[1 + rc * 2 + l]))
        for cp in copies:
            cp.start()
        for cp in copies:
            cp.wait()
        return b

    def place(into, g, which):
        slot = lax.broadcasted_iota(jnp.int32, (tokens, cap), 1).astype(F32)
        for k in range(4):
            r = 4 * g + k
            at0, at1 = colv[:, r:r + 1], colv[:, 16 + r:17 + r]
            at = (at0, at1, jnp.maximum(at0, at1))[which]
            into[:, pl.ds(k * cap, cap)] = jnp.where(slot == at, 1.0, 0.0).astype(BF16)

    def combine_dx(g):
        place(tri, g, 2)
        b = returned(dxr, rdx, g, rdx_r)

        @pl.loop(0, NCOL)
        def _(n):
            at = col(n)
            got = jnp.dot(tri[...], stage_buf[b, :, at], preferred_element_type=F32)
            if g > 0:
                got = acc[0, :, at] + got
            if g < 3:
                acc[0, :, at] = got
            else:
                stage_buf[1 - b, :, at] = got.astype(BF16)
        if g == 3:
            cp = pltpu.make_async_copy(stage_buf.at[1 - b], dxs, misc_sem.at[1])
            cp.start()
            cp.wait()
            for part in range(PARTS):
                push(piece(dxs, part), piece(dx_out, part), z_s.at[part], z_r.at[part], s_prev, 0)

    def combine_y(g):
        for j in range(2):
            place(ext.at[0, j], g, j)
        b = returned(orr, ro, g, ro_r)

        @pl.loop(0, NCOL)
        def _(n):
            at = col(n)
            got = [jnp.dot(ext[0, j], stage_buf[b, :, at], preferred_element_type=F32) for j in range(2)]
            if g > 0:
                got = [acc[j, :, at] + got[j] for j in range(2)]
            if g < 3:
                for j in range(2):
                    acc[j, :, at] = got[j]
            else:
                stage_buf[1 - b, :, at] = (colv[:, 32:33] * got[0] + colv[:, 33:34] * got[1]).astype(BF16)
        if g == 3:
            cp = pltpu.make_async_copy(stage_buf.at[1 - b], y_out, misc_sem.at[1])
            cp.start()
            cp.wait()

    weight_grads(0)
    combine_dx(0)
    combine_dx(1)
    combine_dx(2)
    combine_dx(3)
    weight_grads(1)
    for g in range(4):
        combine_y(g)
    for l in range(2):
        for cp in g_copies(l):
            cp.wait()
    for part in range(PARTS):
        landed(piece(dx_out, part), z_r.at[part])
    for cp in sends:
        cp.wait_send()


def solution(mesh):
    stages = mesh.shape["stage"]
    groups = mesh.shape["expert"]
    tok_spec = P("stage", "expert", None)
    w_spec = P("stage", "expert", None, None)

    def device_step(x_act, route_idx, route_gate, w_up, w_lin, w_down, dy_out):
        tokens, width = x_act.shape[1:]
        local = w_up.shape[1]
        cap = 4 * tokens // (local * groups)
        pair = 2 * cap
        meta = jnp.concatenate([route_idx[0].T.astype(F32), route_gate[0].T, jnp.zeros((4, tokens), F32)], axis=0)

        def arr(*shape, dtype=BF16):
            return jax.ShapeDtypeStruct(shape, dtype)

        def dma(*shape):
            return pltpu.SemaphoreType.DMA(shape)

        tok, weight = arr(tokens, width), arr(local, width, width)
        by_half, by_chip = arr(local, 2, 2 * pair, width), arr(local, 4, pair, width)
        vm = pltpu.VMEM
        outs = pl.pallas_call(
            functools.partial(moe_kernel, stages),
            out_shape=[tok, tok, weight, weight, weight,
                       arr(8, tokens, width), arr(8, tokens, width), arr(8, pair, width), arr(8, pair, width),
                       *[by_half] * 5, by_chip, by_chip, arr(local, 4, 2, pair, width, dtype=F32), tok],
            in_specs=[ANY] * 6,
            out_specs=[ANY] * 18,
            scratch_shapes=[
                *[vm((local, width, width), BF16)] * 3,
                vm((8, 8, tokens), F32), vm((16, tokens), F32), vm((16, tokens), F32), vm((128, tokens), F32), vm((tokens, 128), F32),
                vm((tokens, tokens), BF16), vm((pair, tokens), BF16), vm((pair, 1), F32),
                vm((2, tokens, width), BF16), vm((local, 2, pair, width), F32),
                *[vm((local, pair, width), BF16)] * 4, vm((pair, width // NCOL), BF16), *[vm((local, pair, width), BF16)] * 3,
                vm((2, 2, tokens, width), BF16), vm((2, tokens, width), F32),
                dma(8), dma(8), dma(8, PARTS), dma(8, PARTS), dma(8, PARTS), dma(8, PARTS),
                dma(8, 2), dma(8, 2), dma(8, 2), dma(8, 2), dma(PARTS), dma(PARTS),
                dma(3), dma(2), dma(3, 2), dma(4, 2), dma(2), dma(2), dma(5), dma(2, 3, 2), dma(5),
            ],
            compiler_params=pltpu.CompilerParams(has_side_effects=True, vmem_limit_bytes=63 * 1024 * 1024),
            name="moe_layer",
        )(x_act[0], dy_out[0], meta, w_up[0], w_lin[0], w_down[0])
        return tuple(o[None] for o in outs[:5])

    return jax.shard_map(device_step, mesh=mesh, in_specs=(tok_spec, tok_spec, tok_spec, w_spec, w_spec, w_spec, tok_spec), out_specs=(tok_spec, tok_spec, w_spec, w_spec, w_spec), check_vma=False)
```

```python
import functools

import jax
import jax.numpy as jnp
from jax import lax
from jax.experimental import pallas as pl
from jax.experimental.pallas import tpu as pltpu
from jax.sharding import PartitionSpec as P

F32 = jnp.float32
BF16 = jnp.bfloat16
ANY = pl.BlockSpec(memory_space=pl.ANY)
TN = (((0,), (0,)), ((), ()))
PARTS = 4
NCOL = 4


def moe_kernel(stages, x_in, dy_in, meta_in, wu_in, wl_in, wd_in,
               y_out, dx_out, gu_out, gl_out, gd_out,
               xb, dyb, rdx, ro, xr, dr, hr, dar, dbr, dxr, orr, abr, dxs,
               wu, wl, wd, metab, posv, gatev, rowv, colv, tri, oh, sg, stage_buf, ab,
               xg, hb, ob, dgb, dhb, dab, dbb, dxb, ext, wdt, dx_acc,
               meta_s, meta_r, dy_s, dy_r, x_s, x_r, rdx_s, rdx_r, ro_s, ro_r, z_s, z_r,
               w_sem, load_sem, f_sem, b_sem, ab_out, ab_in, g_load, g_out, misc_sem):
    tokens, width = x_in.shape
    cap = oh.shape[0] // 2
    pair = 2 * cap
    cols = width // NCOL
    wut, wlt = ext.at[0], ext.at[1]
    rows = tokens // PARTS
    s = lax.axis_index("stage")
    e = lax.axis_index("expert")
    y, x, c = e // 4, (e // 2) % 2, e % 2
    s_next = (s + 1) % stages
    s_prev = (s + stages - 1) % stages

    def flip(mask):
        return 1 - y if mask & 4 else y, 1 - x if mask & 2 else x, 1 - c if mask & 1 else c

    def peer(mask):
        py, px, pc = flip(mask)
        return py * 4 + px * 2 + pc

    def rcopy(src, dst, ssem, rsem, stage, mask):
        return pltpu.make_async_remote_copy(src_ref=src, dst_ref=dst, send_sem=ssem, recv_sem=rsem,
                                            device_id={"stage": stage, "expert": peer(mask)}, device_id_type=pl.DeviceIdType.MESH)

    sends = []

    def push(src, dst, ssem, rsem, stage, mask):
        cp = rcopy(src, dst, ssem, rsem, stage, mask)
        cp.start()
        sends.append(cp)

    def landed(dst, rsem):
        rcopy(dst, dst, misc_sem.at[0], rsem, s, 0).wait_recv()

    def piece(ref, part):
        return ref.at[pl.ds(part * rows, rows)]

    def send(src, buf, slot, part, ssem, rsem, stage, mask):
        push(piece(src, part), piece(buf.at[slot], part), ssem.at[slot, part], rsem.at[slot, part], stage, mask)

    def arrive(buf, slot, part, rsem):
        landed(piece(buf.at[slot], part), rsem.at[slot, part])

    def arrive_all(buf, slot, rsem):
        for part in range(PARTS):
            arrive(buf, slot, part, rsem)

    def relay(buf, part, ssem, rsem):
        for m, other, own_half in ((2, 4, part < PARTS // 2), (4, 2, part >= PARTS // 2)):
            arrive(buf, m, part, rsem)
            if own_half:
                send(buf.at[m], buf, 6, part, ssem, rsem, s, other)
            send(buf.at[m], buf, m + 1, part, ssem, rsem, s, 1)

    def relay_diag(buf, part, ssem, rsem):
        arrive(buf, 6, part, rsem)
        send(buf.at[6], buf, 7, part, ssem, rsem, s, 1)

    def col(n):
        return pl.ds(pl.multiple_of(n * cols, cols), cols)

    def row_of(rc):
        return pl.multiple_of((1 - c if rc else c) * cap, cap)

    def own_rows(ref, l, g, rc):
        py, px, _ = flip(2 * g)
        return ref.at[l, py * 2 + px, pl.ds(row_of(rc), cap)]

    def chip_rows(ref, l, g):
        py, px, _ = flip(2 * g)
        if ref.shape[1] == 4:
            return ref.at[l, py * 2 + px]
        return ref.at[l, py, pl.ds(pl.multiple_of(px * pair, pair), pair)]

    for m in range(8):
        push(meta_in, metab.at[m], meta_s.at[m], meta_r.at[m], s_next, m)
    def send_z(part):
        send(x_in, xb, 0, part, x_s, x_r, s_next, 0)

    send_z(0)
    for m in (2, 4):
        send(dy_in, dyb, m, 0, dy_s, dy_r, s, m)
    send_z(1)
    for part in range(PARTS):
        send(dy_in, dyb, 1, part, dy_s, dy_r, s, 1)
    w_loads = [pltpu.make_async_copy(src, dst, w_sem.at[i]) for i, (src, dst) in enumerate(((wu_in, wu), (wl_in, wl), (wd_in, wd)))]
    for cp in w_loads:
        cp.start()

    t_row = lax.broadcasted_iota(jnp.int32, (tokens, tokens), 0)
    t_col = lax.broadcasted_iota(jnp.int32, (tokens, tokens), 1)
    tri[...] = (t_row < t_col).astype(F32).astype(BF16)
    for m in range(8):
        landed(metab.at[m], meta_r.at[m])
    id0, id1, g0, g1 = (metab[:, k, :] for k in range(4))
    for l in range(2):
        mine = (e * 2 + l).astype(F32)
        in0, in1 = id0 == mine, id1 == mine
        gatev[pl.ds(l * 8, 8), :] = jnp.where(in0, g0, 0.0) + jnp.where(in1, g1, 0.0)
        posv[pl.ds(l * 8, 8), :] = jnp.where(in0 | in1, 1.0, 0.0)
    memb = posv[...]
    earlier = jnp.dot(memb.astype(BF16), tri[...], preferred_element_type=F32)
    posv[...] = jnp.where(memb > 0.5, earlier, -1.0)

    def owner_routing():
        rowv[...] = jnp.zeros_like(rowv)
        o0, o1 = metab[0, 0:1, :], metab[0, 1:2, :]
        experts = [(peer(m) * 2 + l).astype(F32) for m in range(8) for l in range(2)]
        for r, mine in enumerate(experts):
            rowv[pl.ds(r, 1), :] = jnp.where((o0 == mine) | (o1 == mine), 1.0, 0.0)
        before = jnp.dot(rowv[pl.ds(0, 16), :].astype(BF16), tri[...], preferred_element_type=F32)
        for r, mine in enumerate(experts):
            rowv[pl.ds(r, 1), :] = jnp.where(o0 == mine, before[r:r + 1], -1.0)
            rowv[pl.ds(16 + r, 1), :] = jnp.where(o1 == mine, before[r:r + 1], -1.0)
        rowv[pl.ds(32, 2), :] = metab[0, 2:4, :]
        colv[...] = rowv[...].T

    def one_hot(m, with_gate):
        slot = lax.broadcasted_iota(jnp.int32, (cap, tokens), 0).astype(F32)
        for l in range(2):
            hit = slot == posv[pl.ds(l * 8 + m, 1), :]
            oh[pl.ds(l * cap, cap), :] = jnp.where(hit, 1.0, 0.0).astype(BF16)
            if with_gate:
                sg[pl.ds(l * cap, cap), :] = jnp.sum(jnp.where(hit, gatev[pl.ds(l * 8 + m, 1), :], 0.0), axis=1, keepdims=True)

    def load(src, buf):
        return pltpu.make_async_copy(src, stage_buf.at[buf], load_sem.at[buf])

    def gather(buf, own, g, into, with_gate):
        srcs = [own if (2 * g + rc == 0 and own is not None) else buf.at[2 * g + rc] for rc in range(2)]
        for rc in range(2):
            load(srcs[rc], rc).start()
        for rc in range(2):
            one_hot(2 * g + rc, with_gate)
            load(srcs[rc], rc).wait()

            @pl.loop(0, NCOL)
            def _(n):
                at = col(n)
                got = jnp.dot(oh[...], stage_buf[rc, :, at], preferred_element_type=F32)
                if with_gate:
                    got = sg[...] * got
                got = got.astype(BF16)
                for l in range(2):
                    into[l, pl.ds(row_of(rc), cap), at] = got[l * cap:(l + 1) * cap]

    def f_outs(g, l):
        return [pltpu.make_async_copy(buf.at[l], chip_rows(out, l, g), f_sem.at[k, l]) for k, (buf, out) in enumerate(((xg, xr), (hb, hr), (ob, orr)))]

    def b_outs(g, l):
        return [pltpu.make_async_copy(buf.at[l], chip_rows(out, l, g), b_sem.at[k, l]) for k, (buf, out) in enumerate(((dgb, dr), (dab, dar), (dbb, dbr), (dxb, dxr)))]

    def ab_store(g, l):
        return pltpu.make_async_copy(ab.at[l], abr.at[l, g], ab_out.at[l])

    def ab_load(g, l):
        return pltpu.make_async_copy(abr.at[l, g], ab.at[l], ab_in.at[l])

    def wait_f(g):
        for l in range(2):
            for cp in f_outs(g, l):
                cp.wait()
            ab_store(g, l).wait()

    def forward(g):
        if g > 0:
            wait_f(g - 1)
        gather(xb, None, g, xg, False)
        for l in range(2):
            @pl.loop(0, NCOL)
            def _(n):
                at = col(n)
                a = jnp.dot(xg[l], wu[l, :, at], preferred_element_type=F32)
                b = jnp.dot(xg[l], wl[l, :, at], preferred_element_type=F32)
                ab[l, 0, :, at] = a
                ab[l, 1, :, at] = b
                hb[l, :, at] = (a * jax.nn.sigmoid(a) * b).astype(BF16)
            ab_store(g, l).start()

            @pl.loop(0, NCOL)
            def _(n):
                at = col(n)
                ob[l, :, at] = jnp.dot(hb[l], wd[l, :, at], preferred_element_type=F32).astype(BF16)
            for cp in f_outs(g, l):
                cp.start()

    def send_back(rows_ref, into, chips, ssem, rsem):
        for l in range(2):
            for m, g, rc in ((2 * g + rc, g, rc) for rc in range(2) for g in chips):
                if m:
                    push(own_rows(rows_ref, l, g, rc), into.at[m, pl.ds(l * cap, cap)], ssem.at[m, l], rsem.at[m, l], s, m)

    def backward(before, g, after):
        if before is None:
            for l in range(2):
                ab_load(g, l).start()
        else:
            for l in range(2):
                for cp in b_outs(before, l)[:3]:
                    cp.wait()
        gather(dyb, dy_in, g, dgb, True)
        for l in range(2):
            ab_load(g, l).wait()

            @pl.loop(0, NCOL)
            def _(n):
                at = col(n)
                dhb[...] = jnp.dot(dgb[l], wdt[l, :, at], preferred_element_type=F32).astype(BF16)
                d_hid = dhb[...].astype(F32)
                a, b = ab[l, 0, :, at], ab[l, 1, :, at]
                sig = jax.nn.sigmoid(a)
                dab[l, :, at] = (d_hid * b * sig * (1.0 + a * (1.0 - sig))).astype(BF16)
                dbb[l, :, at] = (d_hid * (a * sig)).astype(BF16)
            if after is not None:
                ab_load(after, l).start()

            @pl.loop(0, NCOL)
            def _(n):
                at = col(n)
                dxb[l, :, at] = (jnp.dot(dab[l], wut[l, :, at], preferred_element_type=F32)
                                 + jnp.dot(dbb[l], wlt[l, :, at], preferred_element_type=F32)).astype(BF16)
            for cp in b_outs(g, l):
                cp.start()
        for l in range(2):
            b_outs(g, l)[3].wait()

    def transpose(src, dst):
        @pl.loop(0, 2 * NCOL)
        def _(i):
            at = col(i % NCOL)
            dst[i // NCOL, at, :] = src[i // NCOL, :, at].T

    for cp in w_loads:
        cp.wait()
    for part in range(PARTS):
        if part < 3:
            transpose(*((wd, wdt), (wu, wut), (wl, wlt))[part])
        arrive(xb, 0, part, x_r)
        if part + 2 < PARTS:
            send_z(part + 2)
        for m in (2, 4, 1):
            send(xb.at[0], xb, m, part, x_s, x_r, s, m)
        if part > 0:
            relay(xb, part - 1, x_s, x_r)
    for m in (2, 4):
        send(dy_in, dyb, m, 1, dy_s, dy_r, s, m)
    owner_routing()
    relay(xb, PARTS - 1, x_s, x_r)
    for part in (2, 3):
        for m in (2, 4):
            send(dy_in, dyb, m, part, dy_s, dy_r, s, m)
    arrive_all(xb, 1, x_r)
    forward(0)
    relay_diag(xb, 0, x_s, x_r)
    relay_diag(xb, 2, x_s, x_r)
    relay(dyb, 0, dy_s, dy_r)
    arrive_all(xb, 3, x_r)
    forward(1)
    relay_diag(xb, 1, x_s, x_r)
    relay_diag(xb, 3, x_s, x_r)
    arrive_all(xb, 5, x_r)
    forward(2)
    relay(dyb, 1, dy_s, dy_r)
    arrive_all(xb, 7, x_r)
    forward(3)
    relay(dyb, 2, dy_s, dy_r)
    wait_f(3)
    relay(dyb, 3, dy_s, dy_r)
    send_back(orr, ro, (1, 2), ro_s, ro_r)
    arrive_all(dyb, 3, dy_r)
    backward(None, 1, 2)
    relay_diag(dyb, 0, dy_s, dy_r)
    relay_diag(dyb, 1, dy_s, dy_r)
    arrive_all(dyb, 5, dy_r)
    backward(1, 2, 3)
    relay_diag(dyb, 2, dy_s, dy_r)
    relay_diag(dyb, 3, dy_s, dy_r)
    send_back(dxr, rdx, (1, 2), rdx_s, rdx_r)
    arrive_all(dyb, 7, dy_r)
    backward(2, 3, 0)
    send_back(dxr, rdx, (3,), rdx_s, rdx_r)
    send_back(orr, ro, (3, 0), ro_s, ro_r)
    arrive_all(dyb, 1, dy_r)
    backward(3, 0, None)
    send_back(dxr, rdx, (0,), rdx_s, rdx_r)
    for l in range(2):
        for cp in b_outs(0, l)[:3]:
            cp.wait()

    def g_copies(l):
        bufs = (xg, hb, ob) if l == 0 else (dgb, dab, dbb)
        return [pltpu.make_async_copy(buf.at[half], out.at[l, pl.ds(half * pair, pair)], g_out.at[l, k, half])
                for k, (buf, out) in enumerate(zip(bufs, (gu_out, gl_out, gd_out))) for half in range(2)]

    def weight_grads(l):
        loads = [pltpu.make_async_copy(src.at[l], dst, g_load.at[k]) for k, (src, dst) in enumerate(((xr, wu), (dar, ext.at[0]), (dbr, ext.at[1]), (hr, wl), (dr, wd)))]
        for cp in loads:
            cp.start()
        bufs = (xg, hb, ob) if l == 0 else (dgb, dab, dbb)
        block = pair // 2
        for k, (lhs, rhs, need) in enumerate(((wu, ext.at[0], loads[:2]), (wu, ext.at[1], loads[2:3]), (wl, wd, loads[3:]))):
            for cp in need:
                cp.wait()

            @pl.loop(0, width // block)
            def _(i):
                at = pl.ds(pl.multiple_of(i * block, block), block)
                total = (lax.dot_general(lhs[0, :, at], rhs[0], TN, preferred_element_type=F32)
                         + lax.dot_general(lhs[1, :, at], rhs[1], TN, preferred_element_type=F32))
                bufs[k][i // 2, pl.ds(pl.multiple_of(i % 2 * block, block), block), :] = total.astype(BF16)
        for cp in g_copies(l):
            cp.start()

    def returned(rows_ref, into, g, rsem):
        b = g % 2
        for m in (2 * g, 2 * g + 1):
            if m:
                for l in range(2):
                    landed(into.at[m, pl.ds(l * cap, cap)], rsem.at[m, l])
        copies = []
        for rc in range(2):
            m = 2 * g + rc
            for l in range(2):
                src = into.at[m, pl.ds(l * cap, cap)] if m else own_rows(rows_ref, l, 0, 0)
                copies.append(pltpu.make_async_copy(src, stage_buf.at[b, pl.ds((rc * 2 + l) * cap, cap)], misc_sem.at[1 + rc * 2 + l]))
        for cp in copies:
            cp.start()
        for cp in copies:
            cp.wait()
        return b

    def place(into, g, which):
        slot = lax.broadcasted_iota(jnp.int32, (tokens, cap), 1).astype(F32)
        for k in range(4):
            r = 4 * g + k
            at0, at1 = colv[:, r:r + 1], colv[:, 16 + r:17 + r]
            at = (at0, at1, jnp.maximum(at0, at1))[which]
            into[:, pl.ds(k * cap, cap)] = jnp.where(slot == at, 1.0, 0.0).astype(BF16)

    def combine_dx(g):
        place(tri, g, 2)
        b = returned(dxr, rdx, g, rdx_r)

        @pl.loop(0, NCOL)
        def _(n):
            at = col(n)
            got = jnp.dot(tri[...], stage_buf[b, :, at], preferred_element_type=F32)
            if g > 0:
                got = dx_acc[:, at] + got
            if g < 3:
                dx_acc[:, at] = got
            else:
                stage_buf[1 - b, :, at] = got.astype(BF16)
        if g == 3:
            cp = pltpu.make_async_copy(stage_buf.at[1 - b], dxs, misc_sem.at[1])
            cp.start()
            cp.wait()
            for part in range(PARTS):
                push(piece(dxs, part), piece(dx_out, part), z_s.at[part], z_r.at[part], s_prev, 0)

    def combine_y(g):
        for j in range(2):
            place(ext.at[0, j], g, j)
        b = returned(orr, ro, g, ro_r)

        @pl.loop(0, NCOL)
        def _(n):
            at = col(n)
            for half in range(2):
                rs = slice(half * pair, (half + 1) * pair)
                got = [jnp.dot(ext[0, j, rs, :], stage_buf[b, :, at], preferred_element_type=F32) for j in range(2)]
                if g > 0:
                    got = [ab[j, half, :, at] + got[j] for j in range(2)]
                if g < 3:
                    for j in range(2):
                        ab[j, half, :, at] = got[j]
                else:
                    stage_buf[1 - b, rs, at] = (colv[rs, 32:33] * got[0] + colv[rs, 33:34] * got[1]).astype(BF16)
        if g == 3:
            cp = pltpu.make_async_copy(stage_buf.at[1 - b], y_out, misc_sem.at[1])
            cp.start()
            cp.wait()

    weight_grads(0)
    weight_grads(1)
    for g in range(3):
        combine_y(g)
    for g in range(4):
        combine_dx(g)
    combine_y(3)
    for l in range(2):
        for cp in g_copies(l):
            cp.wait()
    for part in range(PARTS):
        landed(piece(dx_out, part), z_r.at[part])
    for cp in sends:
        cp.wait_send()


def solution(mesh):
    stages = mesh.shape["stage"]
    groups = mesh.shape["expert"]
    tok_spec = P("stage", "expert", None)
    w_spec = P("stage", "expert", None, None)

    def device_step(x_act, route_idx, route_gate, w_up, w_lin, w_down, dy_out):
        tokens, width = x_act.shape[1:]
        local = w_up.shape[1]
        cap = 4 * tokens // (local * groups)
        pair = 2 * cap
        meta = jnp.concatenate([route_idx[0].T.astype(F32), route_gate[0].T, jnp.zeros((4, tokens), F32)], axis=0)

        def arr(*shape, dtype=BF16):
            return jax.ShapeDtypeStruct(shape, dtype)

        def dma(*shape):
            return pltpu.SemaphoreType.DMA(shape)

        tok, weight = arr(tokens, width), arr(local, width, width)
        by_half, by_chip = arr(local, 2, 2 * pair, width), arr(local, 4, pair, width)
        vm = pltpu.VMEM
        outs = pl.pallas_call(
            functools.partial(moe_kernel, stages),
            out_shape=[tok, tok, weight, weight, weight,
                       arr(8, tokens, width), arr(8, tokens, width), arr(8, pair, width), arr(8, pair, width),
                       *[by_half] * 5, by_chip, by_chip, arr(local, 4, 2, pair, width, dtype=F32), tok],
            in_specs=[ANY] * 6,
            out_specs=[ANY] * 18,
            scratch_shapes=[
                *[vm((local, width, width), BF16)] * 3,
                vm((8, 8, tokens), F32), vm((16, tokens), F32), vm((16, tokens), F32), vm((128, tokens), F32), vm((tokens, 128), F32),
                vm((tokens, tokens), BF16), vm((pair, tokens), BF16), vm((pair, 1), F32),
                vm((2, tokens, width), BF16), vm((local, 2, pair, width), F32),
                *[vm((local, pair, width), BF16)] * 4, vm((pair, width // NCOL), BF16), *[vm((local, pair, width), BF16)] * 3,
                vm((2, 2, tokens, width), BF16), vm((local, width, width), BF16), vm((tokens, width), F32),
                dma(8), dma(8), dma(8, PARTS), dma(8, PARTS), dma(8, PARTS), dma(8, PARTS),
                dma(8, 2), dma(8, 2), dma(8, 2), dma(8, 2), dma(PARTS), dma(PARTS),
                dma(3), dma(2), dma(3, 2), dma(4, 2), dma(2), dma(2), dma(5), dma(2, 3, 2), dma(5),
            ],
            compiler_params=pltpu.CompilerParams(has_side_effects=True, vmem_limit_bytes=63 * 1024 * 1024),
            name="moe_layer",
        )(x_act[0], dy_out[0], meta, w_up[0], w_lin[0], w_down[0])
        return tuple(o[None] for o in outs[:5])

    return jax.shard_map(device_step, mesh=mesh, in_specs=(tok_spec, tok_spec, tok_spec, w_spec, w_spec, w_spec, tok_spec), out_specs=(tok_spec, tok_spec, w_spec, w_spec, w_spec), check_vma=False)
```

```python
import functools

import jax
import jax.numpy as jnp
from jax import lax
from jax.experimental import pallas as pl
from jax.experimental.pallas import tpu as pltpu
from jax.sharding import PartitionSpec as P

F32 = jnp.float32
BF16 = jnp.bfloat16
ANY = pl.BlockSpec(memory_space=pl.ANY)
TN = (((0,), (0,)), ((), ()))
PARTS = 4
NCOL = 4


def moe_kernel(stages, x_in, dy_in, meta_in, wu_in, wl_in, wd_in,
               y_out, dx_out, gu_out, gl_out, gd_out,
               xb, dyb, rdx, ro, xr, dr, hr, dar, dbr, dxr, orr, abr, dxs,
               wu, wl, wd, metab, posv, gatev, rowv, colv, tri, oh, sg, stage_buf, ab,
               xg, hb, ob, dgb, dhb, dab, dbb, dxb, ext, wdt, dx_acc,
               meta_s, meta_r, dy_s, dy_r, x_s, x_r, rdx_s, rdx_r, ro_s, ro_r, z_s, z_r,
               w_sem, load_sem, f_sem, b_sem, ab_out, ab_in, g_load, g_out, misc_sem):
    tokens, width = x_in.shape
    cap = oh.shape[0] // 2
    pair = 2 * cap
    cols = width // NCOL
    wut, wlt = ext.at[0], ext.at[1]
    rows = tokens // PARTS
    s = lax.axis_index("stage")
    e = lax.axis_index("expert")
    y, x, c = e // 4, (e // 2) % 2, e % 2
    s_next = (s + 1) % stages
    s_prev = (s + stages - 1) % stages

    def flip(mask):
        return 1 - y if mask & 4 else y, 1 - x if mask & 2 else x, 1 - c if mask & 1 else c

    def peer(mask):
        py, px, pc = flip(mask)
        return py * 4 + px * 2 + pc

    def rcopy(src, dst, ssem, rsem, stage, mask):
        return pltpu.make_async_remote_copy(src_ref=src, dst_ref=dst, send_sem=ssem, recv_sem=rsem,
                                            device_id={"stage": stage, "expert": peer(mask)}, device_id_type=pl.DeviceIdType.MESH)

    sends = []

    def push(src, dst, ssem, rsem, stage, mask):
        cp = rcopy(src, dst, ssem, rsem, stage, mask)
        cp.start()
        sends.append(cp)

    def landed(dst, rsem):
        rcopy(dst, dst, misc_sem.at[0], rsem, s, 0).wait_recv()

    def piece(ref, part):
        return ref.at[pl.ds(part * rows, rows)]

    def send(src, buf, slot, part, ssem, rsem, stage, mask):
        push(piece(src, part), piece(buf.at[slot], part), ssem.at[slot, part], rsem.at[slot, part], stage, mask)

    def arrive(buf, slot, part, rsem):
        landed(piece(buf.at[slot], part), rsem.at[slot, part])

    def arrive_all(buf, slot, rsem):
        for part in range(PARTS):
            arrive(buf, slot, part, rsem)

    def relay(buf, part, ssem, rsem):
        for m, other, own_half in ((2, 4, part < PARTS // 2), (4, 2, part >= PARTS // 2)):
            arrive(buf, m, part, rsem)
            if own_half:
                send(buf.at[m], buf, 6, part, ssem, rsem, s, other)
            send(buf.at[m], buf, m + 1, part, ssem, rsem, s, 1)

    def relay_dy(step):
        for m, other, part in ((2, 4, step), (4, 2, (step + PARTS // 2) % PARTS)):
            arrive(dyb, m, part, dy_r)
            if step < PARTS // 2:
                send(dyb.at[m], dyb, 6, part, dy_s, dy_r, s, other)
            send(dyb.at[m], dyb, m + 1, part, dy_s, dy_r, s, 1)

    def relay_diag(buf, part, ssem, rsem):
        arrive(buf, 6, part, rsem)
        send(buf.at[6], buf, 7, part, ssem, rsem, s, 1)

    def col(n):
        return pl.ds(pl.multiple_of(n * cols, cols), cols)

    def row_of(rc):
        return pl.multiple_of((1 - c if rc else c) * cap, cap)

    def own_rows(ref, l, g, rc):
        py, px, _ = flip(2 * g)
        return ref.at[l, py * 2 + px, pl.ds(row_of(rc), cap)]

    def chip_rows(ref, l, g):
        py, px, _ = flip(2 * g)
        if ref.shape[1] == 4:
            return ref.at[l, py * 2 + px]
        return ref.at[l, py, pl.ds(pl.multiple_of(px * pair, pair), pair)]

    for m in range(8):
        push(meta_in, metab.at[m], meta_s.at[m], meta_r.at[m], s_next, m)
    def send_z(part):
        send(x_in, xb, 0, part, x_s, x_r, s_next, 0)

    def send_dy(step):
        for m, part in ((2, step), (4, (step + PARTS // 2) % PARTS)):
            send(dy_in, dyb, m, part, dy_s, dy_r, s, m)

    send_z(0)
    send_dy(0)
    send_z(1)
    for part in range(PARTS):
        send(dy_in, dyb, 1, part, dy_s, dy_r, s, 1)
    w_loads = [pltpu.make_async_copy(src, dst, w_sem.at[i]) for i, (src, dst) in enumerate(((wu_in, wu), (wl_in, wl), (wd_in, wd)))]
    for cp in w_loads:
        cp.start()

    t_row = lax.broadcasted_iota(jnp.int32, (tokens, tokens), 0)
    t_col = lax.broadcasted_iota(jnp.int32, (tokens, tokens), 1)
    tri[...] = (t_row < t_col).astype(F32).astype(BF16)
    for m in range(8):
        landed(metab.at[m], meta_r.at[m])
    id0, id1, g0, g1 = (metab[:, k, :] for k in range(4))
    for l in range(2):
        mine = (e * 2 + l).astype(F32)
        in0, in1 = id0 == mine, id1 == mine
        gatev[pl.ds(l * 8, 8), :] = jnp.where(in0, g0, 0.0) + jnp.where(in1, g1, 0.0)
        posv[pl.ds(l * 8, 8), :] = jnp.where(in0 | in1, 1.0, 0.0)
    memb = posv[...]
    earlier = jnp.dot(memb.astype(BF16), tri[...], preferred_element_type=F32)
    posv[...] = jnp.where(memb > 0.5, earlier, -1.0)

    def owner_routing():
        rowv[...] = jnp.zeros_like(rowv)
        o0, o1 = metab[0, 0:1, :], metab[0, 1:2, :]
        experts = [(peer(m) * 2 + l).astype(F32) for m in range(8) for l in range(2)]
        for r, mine in enumerate(experts):
            rowv[pl.ds(r, 1), :] = jnp.where((o0 == mine) | (o1 == mine), 1.0, 0.0)
        before = jnp.dot(rowv[pl.ds(0, 16), :].astype(BF16), tri[...], preferred_element_type=F32)
        for r, mine in enumerate(experts):
            rowv[pl.ds(r, 1), :] = jnp.where(o0 == mine, before[r:r + 1], -1.0)
            rowv[pl.ds(16 + r, 1), :] = jnp.where(o1 == mine, before[r:r + 1], -1.0)
        rowv[pl.ds(32, 2), :] = metab[0, 2:4, :]
        colv[...] = rowv[...].T

    def one_hot(m, with_gate):
        slot = lax.broadcasted_iota(jnp.int32, (cap, tokens), 0).astype(F32)
        for l in range(2):
            hit = slot == posv[pl.ds(l * 8 + m, 1), :]
            oh[pl.ds(l * cap, cap), :] = jnp.where(hit, 1.0, 0.0).astype(BF16)
            if with_gate:
                sg[pl.ds(l * cap, cap), :] = jnp.sum(jnp.where(hit, gatev[pl.ds(l * 8 + m, 1), :], 0.0), axis=1, keepdims=True)

    def load(src, buf):
        return pltpu.make_async_copy(src, stage_buf.at[buf], load_sem.at[buf])

    def gather(buf, own, g, into, with_gate):
        srcs = [own if (2 * g + rc == 0 and own is not None) else buf.at[2 * g + rc] for rc in range(2)]
        for rc in range(2):
            load(srcs[rc], rc).start()
        for rc in range(2):
            one_hot(2 * g + rc, with_gate)
            load(srcs[rc], rc).wait()

            @pl.loop(0, NCOL)
            def _(n):
                at = col(n)
                got = jnp.dot(oh[...], stage_buf[rc, :, at], preferred_element_type=F32)
                if with_gate:
                    got = sg[...] * got
                got = got.astype(BF16)
                for l in range(2):
                    into[l, pl.ds(row_of(rc), cap), at] = got[l * cap:(l + 1) * cap]

    def f_outs(g, l):
        return [pltpu.make_async_copy(buf.at[l], chip_rows(out, l, g), f_sem.at[k, l]) for k, (buf, out) in enumerate(((xg, xr), (hb, hr), (ob, orr)))]

    def b_outs(g, l):
        return [pltpu.make_async_copy(buf.at[l], chip_rows(out, l, g), b_sem.at[k, l]) for k, (buf, out) in enumerate(((dgb, dr), (dab, dar), (dbb, dbr), (dxb, dxr)))]

    def ab_store(g, l):
        return pltpu.make_async_copy(ab.at[l], abr.at[l, g], ab_out.at[l])

    def ab_load(g, l):
        return pltpu.make_async_copy(abr.at[l, g], ab.at[l], ab_in.at[l])

    def wait_f(g):
        for l in range(2):
            for cp in f_outs(g, l):
                cp.wait()
            ab_store(g, l).wait()

    def forward(g):
        if g > 0:
            wait_f(g - 1)
        if g == 3:
            send_back(orr, ro, (1, 2), ro_s, ro_r)
        gather(xb, None, g, xg, False)
        for l in range(2):
            @pl.loop(0, NCOL)
            def _(n):
                at = col(n)
                a = jnp.dot(xg[l], wu[l, :, at], preferred_element_type=F32)
                b = jnp.dot(xg[l], wl[l, :, at], preferred_element_type=F32)
                ab[l, 0, :, at] = a
                ab[l, 1, :, at] = b
                hb[l, :, at] = (a * jax.nn.sigmoid(a) * b).astype(BF16)
            ab_store(g, l).start()

            @pl.loop(0, NCOL)
            def _(n):
                at = col(n)
                ob[l, :, at] = jnp.dot(hb[l], wd[l, :, at], preferred_element_type=F32).astype(BF16)
            for cp in f_outs(g, l):
                cp.start()

    def send_back(rows_ref, into, chips, ssem, rsem):
        for l in range(2):
            for m, g, rc in ((2 * g + rc, g, rc) for rc in range(2) for g in chips):
                if m:
                    push(own_rows(rows_ref, l, g, rc), into.at[m, pl.ds(l * cap, cap)], ssem.at[m, l], rsem.at[m, l], s, m)

    def backward(before, g, after):
        if before is None:
            for l in range(2):
                ab_load(g, l).start()
        else:
            for l in range(2):
                for cp in b_outs(before, l)[:3]:
                    cp.wait()
        gather(dyb, dy_in, g, dgb, True)
        for l in range(2):
            ab_load(g, l).wait()

            @pl.loop(0, NCOL)
            def _(n):
                at = col(n)
                dhb[...] = jnp.dot(dgb[l], wdt[l, :, at], preferred_element_type=F32).astype(BF16)
                d_hid = dhb[...].astype(F32)
                a, b = ab[l, 0, :, at], ab[l, 1, :, at]
                sig = jax.nn.sigmoid(a)
                dab[l, :, at] = (d_hid * b * sig * (1.0 + a * (1.0 - sig))).astype(BF16)
                dbb[l, :, at] = (d_hid * (a * sig)).astype(BF16)
            if after is not None:
                ab_load(after, l).start()

            @pl.loop(0, NCOL)
            def _(n):
                at = col(n)
                dxb[l, :, at] = (jnp.dot(dab[l], wut[l, :, at], preferred_element_type=F32)
                                 + jnp.dot(dbb[l], wlt[l, :, at], preferred_element_type=F32)).astype(BF16)
            for cp in b_outs(g, l):
                cp.start()
        for l in range(2):
            b_outs(g, l)[3].wait()

    def transpose(src, dst):
        @pl.loop(0, 2 * NCOL)
        def _(i):
            at = col(i % NCOL)
            dst[i // NCOL, at, :] = src[i // NCOL, :, at].T

    for cp in w_loads:
        cp.wait()
    for part in range(PARTS):
        if part < 3:
            transpose(*((wd, wdt), (wu, wut), (wl, wlt))[part])
        arrive(xb, 0, part, x_r)
        if part + 2 < PARTS:
            send_z(part + 2)
        for m in (2, 4, 1):
            send(xb.at[0], xb, m, part, x_s, x_r, s, m)
        if part > 0:
            relay(xb, part - 1, x_s, x_r)
    send_dy(1)
    owner_routing()
    relay(xb, PARTS - 1, x_s, x_r)
    send_dy(2)
    send_dy(3)
    arrive_all(xb, 1, x_r)
    forward(0)
    relay_diag(xb, 0, x_s, x_r)
    relay_diag(xb, 2, x_s, x_r)
    relay_dy(0)
    arrive_all(xb, 3, x_r)
    forward(1)
    relay_diag(xb, 1, x_s, x_r)
    relay_diag(xb, 3, x_s, x_r)
    relay_dy(1)
    arrive_all(xb, 5, x_r)
    forward(2)
    arrive_all(xb, 7, x_r)
    forward(3)
    wait_f(3)
    relay_dy(2)
    relay_dy(3)
    arrive_all(dyb, 3, dy_r)
    backward(None, 1, 2)
    relay_diag(dyb, 0, dy_s, dy_r)
    relay_diag(dyb, 2, dy_s, dy_r)
    arrive_all(dyb, 5, dy_r)
    backward(1, 2, 3)
    send_back(dxr, rdx, (1, 2), rdx_s, rdx_r)
    relay_diag(dyb, 1, dy_s, dy_r)
    relay_diag(dyb, 3, dy_s, dy_r)
    arrive_all(dyb, 7, dy_r)
    backward(2, 3, 0)
    send_back(dxr, rdx, (3,), rdx_s, rdx_r)
    send_back(orr, ro, (3, 0), ro_s, ro_r)
    arrive_all(dyb, 1, dy_r)
    backward(3, 0, None)
    send_back(dxr, rdx, (0,), rdx_s, rdx_r)
    for l in range(2):
        for cp in b_outs(0, l)[:3]:
            cp.wait()

    def g_copies(l):
        bufs = (xg, hb, ob) if l == 0 else (dgb, dab, dbb)
        return [pltpu.make_async_copy(buf.at[half], out.at[l, pl.ds(half * pair, pair)], g_out.at[l, k, half])
                for k, (buf, out) in enumerate(zip(bufs, (gu_out, gl_out, gd_out))) for half in range(2)]

    def weight_grads(l):
        loads = [pltpu.make_async_copy(src.at[l], dst, g_load.at[k]) for k, (src, dst) in enumerate(((xr, wu), (dar, ext.at[0]), (dbr, ext.at[1]), (hr, wl), (dr, wd)))]
        for cp in loads:
            cp.start()
        bufs = (xg, hb, ob) if l == 0 else (dgb, dab, dbb)
        block = pair // 2
        for k, (lhs, rhs, need) in enumerate(((wu, ext.at[0], loads[:2]), (wu, ext.at[1], loads[2:3]), (wl, wd, loads[3:]))):
            for cp in need:
                cp.wait()

            @pl.loop(0, width // block)
            def _(i):
                at = pl.ds(pl.multiple_of(i * block, block), block)
                total = (lax.dot_general(lhs[0, :, at], rhs[0], TN, preferred_element_type=F32)
                         + lax.dot_general(lhs[1, :, at], rhs[1], TN, preferred_element_type=F32))
                bufs[k][i // 2, pl.ds(pl.multiple_of(i % 2 * block, block), block), :] = total.astype(BF16)
        for cp in g_copies(l):
            cp.start()

    def returned(rows_ref, into, g, rsem):
        b = g % 2
        for m in (2 * g, 2 * g + 1):
            if m:
                for l in range(2):
                    landed(into.at[m, pl.ds(l * cap, cap)], rsem.at[m, l])
        copies = []
        for rc in range(2):
            m = 2 * g + rc
            for l in range(2):
                src = into.at[m, pl.ds(l * cap, cap)] if m else own_rows(rows_ref, l, 0, 0)
                copies.append(pltpu.make_async_copy(src, stage_buf.at[b, pl.ds((rc * 2 + l) * cap, cap)], misc_sem.at[1 + rc * 2 + l]))
        for cp in copies:
            cp.start()
        for cp in copies:
            cp.wait()
        return b

    def place(into, g, which):
        slot = lax.broadcasted_iota(jnp.int32, (tokens, cap), 1).astype(F32)
        for k in range(4):
            r = 4 * g + k
            at0, at1 = colv[:, r:r + 1], colv[:, 16 + r:17 + r]
            at = (at0, at1, jnp.maximum(at0, at1))[which]
            into[:, pl.ds(k * cap, cap)] = jnp.where(slot == at, 1.0, 0.0).astype(BF16)

    def combine_dx(g):
        place(tri, g, 2)
        b = returned(dxr, rdx, g, rdx_r)

        @pl.loop(0, NCOL)
        def _(n):
            at = col(n)
            got = jnp.dot(tri[...], stage_buf[b, :, at], preferred_element_type=F32)
            if g > 0:
                got = dx_acc[:, at] + got
            if g < 3:
                dx_acc[:, at] = got
            else:
                stage_buf[1 - b, :, at] = got.astype(BF16)
        if g == 3:
            cp = pltpu.make_async_copy(stage_buf.at[1 - b], dxs, misc_sem.at[1])
            cp.start()
            cp.wait()
            for part in range(PARTS):
                push(piece(dxs, part), piece(dx_out, part), z_s.at[part], z_r.at[part], s_prev, 0)

    def combine_y(g):
        for j in range(2):
            place(ext.at[0, j], g, j)
        b = returned(orr, ro, g, ro_r)

        @pl.loop(0, NCOL)
        def _(n):
            at = col(n)
            for half in range(2):
                rs = slice(half * pair, (half + 1) * pair)
                got = [jnp.dot(ext[0, j, rs, :], stage_buf[b, :, at], preferred_element_type=F32) for j in range(2)]
                if g > 0:
                    got = [ab[j, half, :, at] + got[j] for j in range(2)]
                if g < 3:
                    for j in range(2):
                        ab[j, half, :, at] = got[j]
                else:
                    stage_buf[1 - b, rs, at] = (colv[rs, 32:33] * got[0] + colv[rs, 33:34] * got[1]).astype(BF16)
        if g == 3:
            cp = pltpu.make_async_copy(stage_buf.at[1 - b], y_out, misc_sem.at[1])
            cp.start()
            cp.wait()

    weight_grads(0)
    for g in range(3):
        combine_y(g)
    for g in range(4):
        combine_dx(g)
    weight_grads(1)
    combine_y(3)
    for l in range(2):
        for cp in g_copies(l):
            cp.wait()
    for part in range(PARTS):
        landed(piece(dx_out, part), z_r.at[part])
    for cp in sends:
        cp.wait_send()


def solution(mesh):
    stages = mesh.shape["stage"]
    groups = mesh.shape["expert"]
    tok_spec = P("stage", "expert", None)
    w_spec = P("stage", "expert", None, None)

    def device_step(x_act, route_idx, route_gate, w_up, w_lin, w_down, dy_out):
        tokens, width = x_act.shape[1:]
        local = w_up.shape[1]
        cap = 4 * tokens // (local * groups)
        pair = 2 * cap
        meta = jnp.concatenate([route_idx[0].T.astype(F32), route_gate[0].T, jnp.zeros((4, tokens), F32)], axis=0)

        def arr(*shape, dtype=BF16):
            return jax.ShapeDtypeStruct(shape, dtype)

        def dma(*shape):
            return pltpu.SemaphoreType.DMA(shape)

        tok, weight = arr(tokens, width), arr(local, width, width)
        by_half, by_chip = arr(local, 2, 2 * pair, width), arr(local, 4, pair, width)
        vm = pltpu.VMEM
        outs = pl.pallas_call(
            functools.partial(moe_kernel, stages),
            out_shape=[tok, tok, weight, weight, weight,
                       arr(8, tokens, width), arr(8, tokens, width), arr(8, pair, width), arr(8, pair, width),
                       *[by_half] * 5, by_chip, by_chip, arr(local, 4, 2, pair, width, dtype=F32), tok],
            in_specs=[ANY] * 6,
            out_specs=[ANY] * 18,
            scratch_shapes=[
                *[vm((local, width, width), BF16)] * 3,
                vm((8, 8, tokens), F32), vm((16, tokens), F32), vm((16, tokens), F32), vm((128, tokens), F32), vm((tokens, 128), F32),
                vm((tokens, tokens), BF16), vm((pair, tokens), BF16), vm((pair, 1), F32),
                vm((2, tokens, width), BF16), vm((local, 2, pair, width), F32),
                *[vm((local, pair, width), BF16)] * 4, vm((pair, width // NCOL), BF16), *[vm((local, pair, width), BF16)] * 3,
                vm((2, 2, tokens, width), BF16), vm((local, width, width), BF16), vm((tokens, width), F32),
                dma(8), dma(8), dma(8, PARTS), dma(8, PARTS), dma(8, PARTS), dma(8, PARTS),
                dma(8, 2), dma(8, 2), dma(8, 2), dma(8, 2), dma(PARTS), dma(PARTS),
                dma(3), dma(2), dma(3, 2), dma(4, 2), dma(2), dma(2), dma(5), dma(2, 3, 2), dma(5),
            ],
            compiler_params=pltpu.CompilerParams(has_side_effects=True, vmem_limit_bytes=63 * 1024 * 1024),
            name="moe_layer",
        )(x_act[0], dy_out[0], meta, w_up[0], w_lin[0], w_down[0])
        return tuple(o[None] for o in outs[:5])

    return jax.shard_map(device_step, mesh=mesh, in_specs=(tok_spec, tok_spec, tok_spec, w_spec, w_spec, w_spec, tok_spec), out_specs=(tok_spec, tok_spec, w_spec, w_spec, w_spec), check_vma=False)
```
